512 devices in a mesh: gx: 8 (over y, core), gy: 16 (over z), gz: 4 (over x).
Axes of the slice: x: 4, y: 4, z: 16, core: 2. Of those that a mesh axis runs over, the one named last changes fastest.
Arguments:
- a_vals: float32 [16, 16, 4, 6, 128, 128], P('gy', 'gx', 'gz'), may hold values from -0.25 to 0.25
- a_cols: int32 [16, 16, 4, 6], P('gy', 'gx', 'gz'), may hold values from 0 to 63, as said below
- a_count: int32 [16, 16, 4], P('gy', 'gx', 'gz'), may hold values from 1 to 6, as said below
- p_vals: float32 [4, 64, 8, 1, 128, 128], P('gz', 'gy', 'gx'), may hold values from -6 to 6
- p_cols: int32 [4, 64, 8, 1], P('gz', 'gy', 'gx'), may hold values from 0 to 1, as said below
- p_count: int32 [4, 64, 8], P('gz', 'gy', 'gx'), may hold values from 0 to 1, as said below
Outputs:
- c_tiles: float32 [32768, 2048], P(('gy', 'gz'), 'gx')
The draws below stay inside these ranges and needn't reach their ends.
Inputs may be any that keep to these rules, and one draw needn't show every extreme that they name: `a_cols`: inner tile indices of one block row and slice are distinct across its 6 slots. Slots 0 to a_count - 1 are live; the block rows of every device include one with all 6 slots live. `p_cols`: column tiles of one block row and group are distinct across its 1 slots. Slots 0 to p_count - 1 are live; the block rows of every device include one with all 1 slots live.
All inputs are finite; a program needn't handle non-finite values.
Results may differ from the reference program's by a relative error of at most 0.0003.
Values sent between devices are 32-bit elements; how exact they have to be, the bound alone decides.
A program may use at most 128 MiB of HBM per device.

```python
import jax
import jax.numpy as jnp
from jax import lax

TILE = 128
ROWS_DEV = 2
SLOTS_A = 6
SLOTS_P = 1
COLS_DEV = 2
RX = 16
KZ = 64
N_GX = 8
N_GY = 16
N_GZ = 4


def draw_a_count(key, part):
    first = jax.random.randint(jax.random.fold_in(key, 11), (N_GY, RX, N_GZ), 1, SLOTS_A + 1)
    second = jax.random.randint(jax.random.fold_in(key, 12), (N_GY, RX, N_GZ), 1, SLOTS_A + 1)
    counts = jnp.minimum(first, second)
    picked = jax.random.randint(jax.random.fold_in(key, 13), (N_GY, RX // ROWS_DEV, 1, N_GZ), 0, ROWS_DEV)
    position = jnp.arange(ROWS_DEV, dtype=jnp.int32)[None, None, :, None]
    filled = (position == picked).reshape(N_GY, RX, N_GZ)
    return jnp.where(filled, SLOTS_A, counts).astype(jnp.int32)


def draw_a_cols(key, part):
    line_total = N_GY * RX * N_GZ
    base = jnp.broadcast_to(jnp.arange(KZ, dtype=jnp.int32), (line_total, KZ))
    mixed = jax.random.permutation(jax.random.fold_in(key, 21), base, axis=1, independent=True)
    return mixed[:, :SLOTS_A].reshape(N_GY, RX, N_GZ, SLOTS_A).astype(jnp.int32)


def draw_p_count(key, part):
    counts = jax.random.randint(jax.random.fold_in(key, 31), (N_GZ, KZ, N_GX), 0, SLOTS_P + 1)
    block_rows = KZ // N_GY
    picked = jax.random.randint(jax.random.fold_in(key, 32), (N_GZ, N_GY, 1, N_GX), 0, block_rows)
    position = jnp.arange(block_rows, dtype=jnp.int32)[None, None, :, None]
    filled = (position == picked).reshape(N_GZ, KZ, N_GX)
    return jnp.where(filled, SLOTS_P, counts).astype(jnp.int32)


def draw_p_cols(key, part):
    line_total = N_GZ * KZ * N_GX
    base = jnp.broadcast_to(jnp.arange(COLS_DEV, dtype=jnp.int32), (line_total, COLS_DEV))
    mixed = jax.random.permutation(jax.random.fold_in(key, 41), base, axis=1, independent=True)
    return mixed[:, :SLOTS_P].reshape(N_GZ, KZ, N_GX, SLOTS_P).astype(jnp.int32)


def shard_levels(rng, dims, cuts, least, largest):
    loudness = 1.0
    for dim, blocks in cuts:
        steps = jax.random.uniform(jax.random.fold_in(jax.random.fold_in(rng, 6), dim), (blocks,), jnp.float32, least / len(cuts), largest / len(cuts))
        loudness = loudness * jnp.repeat(jnp.exp(steps), dims[dim] // blocks).reshape((-1,) + (1,) * (len(dims) - 1 - dim))
    return loudness


def noise(own_key, shape, width, bound, cuts=(), kind=jnp.bfloat16):
    values = width * jax.random.normal(own_key, shape, jnp.float32)
    if cuts:
        values = values * shard_levels(own_key, shape, cuts, -0.22, 0.18)
    return jnp.clip(values, -bound, bound).astype(kind)


def setup_inputs(seed: int = 0) -> dict:
    key_of = jax.random.split(jax.random.key(seed), 7)
    a_vals = noise(key_of[0], (N_GY, RX, N_GZ, SLOTS_A, TILE, TILE), (4 * TILE) ** -0.5, 0.25, ((0, 16), (1, 8), (2, 4)), jnp.float32)
    a_cols = draw_a_cols(jax.random.fold_in(key_of[6], 71), 0)
    a_count = draw_a_count(jax.random.fold_in(key_of[6], 71), 0)
    p_vals = noise(key_of[3], (N_GZ, KZ, N_GX, SLOTS_P, TILE, TILE), 1.0, 6.0, ((0, 4), (1, 16), (2, 8)), jnp.float32)
    p_cols = draw_p_cols(jax.random.fold_in(key_of[6], 71), 0)
    p_count = draw_p_count(jax.random.fold_in(key_of[6], 71), 0)
    return dict(a_vals=a_vals, a_cols=a_cols, a_count=a_count, p_vals=p_vals, p_cols=p_cols, p_count=p_count)


def reference(a_vals, a_cols, a_count, p_vals, p_cols, p_count):
    tile_size = a_vals.shape[-1]
    groups_y, rows_x, slices, slots_a = a_cols.shape
    inner_rows = p_cols.shape[1]
    groups_x = p_cols.shape[2]
    slots_p = p_cols.shape[3]
    rows_all = groups_y * rows_x
    a_values = a_vals.reshape(rows_all, slices, slots_a, tile_size, tile_size)
    a_columns = a_cols.reshape(rows_all, slices, slots_a)
    a_counts = a_count.reshape(rows_all, slices)
    p_values = p_vals.reshape(slices * inner_rows, groups_x, slots_p, tile_size, tile_size)
    alive_p = jnp.arange(slots_p, dtype=jnp.int32) < p_count[..., None]
    matches = p_cols[..., None] == jnp.arange(COLS_DEV, dtype=jnp.int32)
    p_weights = (alive_p[..., None] & matches).astype(jnp.float32)
    p_weights = p_weights.reshape(slices * inner_rows, groups_x, slots_p, COLS_DEV)
    offsets = (jnp.arange(slices, dtype=jnp.int32) * inner_rows)[:, None]

    def one_row(row_index):
        alive_a = jnp.arange(slots_a, dtype=jnp.int32) < a_counts[row_index][:, None]
        tile_part = jnp.where(alive_a[..., None, None], a_values[row_index], 0.0)
        indices = a_columns[row_index].astype(jnp.int32) + offsets
        chosen = p_values[indices]
        weights = p_weights[indices]
        product = jnp.einsum("zsij,zsxpjk->zsxpik", tile_part, chosen, precision=lax.Precision.HIGHEST)
        placed = jnp.einsum("zsxpc,zsxpik->ixck", weights, product, precision=lax.Precision.HIGHEST)
        return placed.reshape(tile_size, groups_x * COLS_DEV * tile_size)

    result = lax.map(one_row, jnp.arange(rows_all, dtype=jnp.int32))
    return result.reshape(rows_all * tile_size, groups_x * COLS_DEV * tile_size)
```

```python
import jax
import jax.numpy as jnp
from jax import lax
from jax.experimental import pallas as pl
from jax.experimental.pallas import tpu as pltpu
from jax.sharding import PartitionSpec as P

MESH = pl.DeviceIdType.MESH
T = 128
NY = 4
NC = 2
NZ = 16
NX = 4
SLOTS = 6
ROWS_DEV = 2
TILES_A = ROWS_DEV * SLOTS
UNIT = 3
UNITS = TILES_A // UNIT
TILES_P = 4
PROWS = TILES_P * T + 8
HALF = NZ // 2
BF = jnp.bfloat16
F32 = jnp.float32


def kernel(
    a_hbm, ac, an, p_hbm, pc, pn, out_hbm,
    abuf, ameta, ameta_s, pbuf, phi, plo, cbuf, far, near,
    own_sem, p_send, p_recv, a_send, a_recv, m_send, m_recv,
    sib_send, sib_recv, smeta_recv, c_send, far_recv, near_recv, out_sem, meta_sem, go_sem,
):
    gx, me, x = lax.axis_index("gx"), lax.axis_index("gy"), lax.axis_index("gz")
    y, core = gx // NC, gx % NC

    def wrap(value, n):
        return lax.rem(value + 2 * n, n)

    def y_dev(d):
        return {"gx": wrap(y + d, NY) * NC + core}

    def y_slot(d):
        return wrap(y + d, NY) * NC + core

    sibling = {"gx": y * NC + 1 - core}

    def sib_slot(d):
        return wrap(y + d, NY) * NC + 1 - core

    def remote(src, dst, send, recv, device):
        return pltpu.make_async_remote_copy(
            src_ref=src, dst_ref=dst, send_sem=send, recv_sem=recv, device_id=device, device_id_type=MESH
        )

    own_a = pltpu.make_async_copy(a_hbm, abuf.at[gx], own_sem.at[0])
    own_p = pltpu.make_async_copy(p_hbm, pbuf.at[me, pl.ds(0, TILES_P * T)], own_sem.at[1])
    own_a.start()
    own_p.start()

    barrier = pltpu.get_barrier_semaphore()
    peers = [sibling, y_dev(1), y_dev(-1), {"gy": wrap(me + 1, NZ)}, {"gy": wrap(me - 1, NZ)}, {"gz": wrap(x + 1, NX)}, {"gz": wrap(x - 1, NX)}]
    for peer in peers:
        pl.semaphore_signal(barrier, inc=1, device_id=peer, device_id_type=MESH)

    row8 = lax.broadcasted_iota(jnp.int32, (8, T), 0)
    lane8 = lax.broadcasted_iota(jnp.int32, (8, T), 1)
    pmeta = jnp.zeros((8, T), F32)
    for t in range(TILES_P):
        live = pn[0, t, 0] > 0
        for col in range(2):
            weight = jnp.where(jnp.logical_and(live, pc[0, t, 0, 0] == col), 1.0, 0.0).astype(F32)
            pmeta = jnp.where(row8 == col * TILES_P + t, weight, pmeta)
    pbuf[me, TILES_P * T :, :] = pmeta
    meta = jnp.zeros((8, T), jnp.int32)
    for r in range(ROWS_DEV):
        for s in range(SLOTS):
            target = jnp.where(s < an[0, r, 0], ac[0, r, 0, s], NZ * TILES_P)
            meta = jnp.where(lane8 == r * SLOTS + s, target, meta)
    ameta[gx] = meta
    phi[NZ * TILES_P] = jnp.zeros((T, 2 * T), BF)
    plo[NZ * TILES_P] = jnp.zeros((T, 2 * T), BF)

    pl.semaphore_wait(barrier, len(peers))

    def a_part(slot, u, n=1):
        return abuf.at[slot, pl.ds(u * UNIT, n * UNIT)]

    ORDER = {1: (0, 1, 2, 3), -1: (2, 3, 0, 1)}
    EARLY = {1: (0, 1), -1: (2, 3)}
    LATE = {1: (2, 3), -1: (0, 1)}
    DIR = {1: 0, -1: 1}

    def a_first(d, u, slot):
        return remote(a_part(slot, u), a_part(slot, u), a_send.at[DIR[d], 0], a_recv.at[DIR[d], 0, u], y_dev(d))

    def a_second(d, u, slot):
        return remote(a_part(slot, u), a_part(slot, u), a_send.at[DIR[d], 1], a_recv.at[DIR[d], 1, u], y_dev(d))

    def m_first(d, slot):
        return remote(ameta.at[slot], ameta.at[slot], m_send.at[DIR[d]], m_recv.at[DIR[d]], y_dev(d))

    def m_second(slot):
        return remote(ameta.at[slot], ameta.at[slot], m_send.at[2], m_recv.at[2], y_dev(1))

    def to_sibling(kind, u, slot):
        return remote(a_part(slot, u), a_part(slot, u), sib_send.at[0], sib_recv.at[kind, u], sibling)

    def m_sibling(kind, slot):
        return remote(ameta.at[slot], ameta.at[slot], sib_send.at[1], smeta_recv.at[kind], sibling)

    def a_start():
        own_a.wait()
        for i in range(UNITS):
            for d in (1, -1):
                a_first(d, ORDER[d][i], gx).start()
            if i == 0:
                for d in (1, -1):
                    m_first(d, gx).start()
        for u in range(UNITS):
            to_sibling(0, u, gx).start()
        m_sibling(0, gx).start()

    def a_early():
        for i in range(UNITS // 2):
            for d in (1, -1):
                u = EARLY[d][i]
                slot = y_slot(-d)
                a_first(d, u, slot).wait_recv()
                a_second(d, u, slot).start()
                to_sibling(1 + DIR[d], u, slot).start()
            if i == 0:
                for d in (1, -1):
                    slot = y_slot(-d)
                    m_first(d, slot).wait_recv()
                    if d == 1:
                        m_second(slot).start()
                    m_sibling(1 + DIR[d], slot).start()

    def a_late():
        for i in range(UNITS // 2):
            for d in (1, -1):
                u = LATE[d][i]
                slot = y_slot(-d)
                a_first(d, u, slot).wait_recv()
                to_sibling(1 + DIR[d], u, slot).start()

    def a_far():
        slot = y_slot(2)
        m_second(slot).wait_recv()
        m_sibling(3, slot).start()
        for i in range(UNITS // 2):
            for d in (1, -1):
                u = EARLY[d][i]
                a_second(d, u, slot).wait_recv()
                to_sibling(3, u, slot).start()

    def a_finish():
        for kind, d in ((0, 0), (1, -1), (2, 1), (3, 2)):
            slot = sib_slot(d)
            m_sibling(kind, slot).wait_recv()
            for u in range(UNITS):
                to_sibling(kind, u, slot).wait_recv()
        copy = pltpu.make_async_copy(ameta, ameta_s, meta_sem)
        copy.start()
        copy.wait()

    def a_drain():
        for d in (0, 1):
            pltpu.make_async_copy(abuf.at[0], abuf.at[0], a_send.at[d, 0]).wait()
            half = abuf.at[0, pl.ds(0, TILES_A // 2)]
            pltpu.make_async_copy(half, half, a_send.at[d, 1]).wait()
        for j in range(3):
            pltpu.make_async_copy(ameta.at[0], ameta.at[0], m_send.at[j]).wait()
        part = abuf.at[pl.ds(0, NY)]
        pltpu.make_async_copy(part, part, sib_send.at[0]).wait()
        part = ameta.at[pl.ds(0, NY)]
        pltpu.make_async_copy(part, part, sib_send.at[1]).wait()

    PIECES = (3, 0, 1, 2)
    LAST = {1: (0, 1), -1: (3, 2)}

    def p_part(slot, j):
        return pbuf.at[slot, pl.ds(j * T, T + 8 if j == TILES_P - 1 else T)]

    def p_copy(d, step, j, slot, last=False):
        part = p_part(slot, j)
        return remote(
            part, part, p_send.at[DIR[d], 1 if last else 0], p_recv.at[DIR[d], step - 1, j], {"gy": wrap(me + d, NZ)}
        )

    def convert(slot, j):
        p = pbuf[slot, j * T : (j + 1) * T, :]
        weights = pbuf[slot, TILES_P * T :, :].astype(BF)
        hi = p.astype(BF)
        lo = (p - hi.astype(F32)).astype(BF)
        k = slot * TILES_P + j
        for col in range(2):
            weight = weights[col * TILES_P + j : col * TILES_P + j + 1, :]
            phi[k, :, col * T : (col + 1) * T] = hi * weight
            plo[k, :, col * T : (col + 1) * T] = lo * weight

    def p_start():
        own_p.wait()
        for j in PIECES:
            for d in (1, -1):
                p_copy(d, 1, j, me).start()
        for j in range(TILES_P):
            convert(me, j)

    def p_steps(first, last):
        def step(s, carry):
            for j in PIECES:
                for d in (1, -1):
                    slot = wrap(me - d * s, NZ)
                    p_copy(d, s, j, slot).wait_recv()
                    p_copy(d, s + 1, j, slot).start()
                for d in (1, -1):
                    convert(wrap(me - d * s, NZ), j)
            return carry

        lax.fori_loop(first, last + 1, step, 0)

    def p_seven():
        s = HALF - 1
        for j in PIECES:
            for d in (1, -1):
                slot = wrap(me - d * s, NZ)
                p_copy(d, s, j, slot).wait_recv()
                if j in LAST[d]:
                    p_copy(d, HALF, j, slot, last=True).start()
            for d in (1, -1):
                convert(wrap(me - d * s, NZ), j)

    def p_eight():
        slot = wrap(me + HALF, NZ)
        for i in range(TILES_P // 2):
            for d in (1, -1):
                p_copy(d, HALF, LAST[d][i], slot, last=True).wait_recv()
            for d in (1, -1):
                convert(slot, LAST[d][i])

    def p_drain():
        part = pbuf.at[pl.ds(0, HALF - 1)]
        for d in (1, -1):
            pltpu.make_async_copy(part, part, p_send.at[DIR[d], 0]).wait()
            rest = pbuf.at[0, pl.ds(0, 2 * T if d == 1 else 2 * T + 8)]
            pltpu.make_async_copy(rest, rest, p_send.at[DIR[d], 1]).wait()

    @pl.when(core == 0)
    def _():
        p_start()
        a_start()
        p_steps(1, 3)
        a_early()
        p_steps(4, HALF - 2)
        a_late()
        p_seven()
        pl.semaphore_signal(go_sem, inc=1, device_id=sibling, device_id_type=MESH)
        p_eight()
        a_far()

    @pl.when(core == 1)
    def _():
        a_start()
        a_early()
        a_late()
        pl.semaphore_wait(go_sem, 1)
        p_start()
        p_steps(1, 2)
        a_far()
        p_steps(3, HALF - 2)
        p_seven()
        p_eight()

    a_finish()

    def compute(o, b):
        row = o * NX + b
        slot, r = row // ROWS_DEV, row % ROWS_DEV
        total = jnp.zeros((T, 2 * T), F32)
        for pair in range(SLOTS // 2):
            left, high, low = [], [], []
            for s in (2 * pair, 2 * pair + 1):
                k = ameta_s[slot, 0, r * SLOTS + s]
                left.append(abuf[slot, r * SLOTS + s])
                high.append(phi[k])
                low.append(plo[k])
            a = jnp.concatenate(left, axis=1)
            hi = a.astype(BF)
            lo = (a - hi.astype(F32)).astype(BF)
            high = jnp.concatenate(high, axis=0)
            low = jnp.concatenate(low, axis=0)
            total += jnp.dot(hi, high, preferred_element_type=F32)
            total += jnp.dot(lo, high, preferred_element_type=F32)
            total += jnp.dot(hi, low, preferred_element_type=F32)
        cbuf[row] = total

    def c_far(d, h, b):
        return remote(cbuf.at[wrap(x + 2, NX) * NX + b], far.at[DIR[d], h], c_send.at[DIR[d]], far_recv.at[DIR[d], h], {"gz": wrap(x + d, NX)})

    def c_near(d, b):
        return remote(cbuf.at[wrap(x + d, NX) * NX + b], near.at[DIR[d], b], c_send.at[DIR[d]], near_recv.at[DIR[d], b], {"gz": wrap(x + d, NX)})

    opposite, right, left = wrap(x + 2, NX), wrap(x + 1, NX), wrap(x - 1, NX)

    def far_rows(b, carry):
        compute(opposite, b)
        c_far(1, b, b).start()
        compute(opposite, b + 2)
        c_far(-1, b, b + 2).start()
        return carry

    lax.fori_loop(0, 2, far_rows, 0)

    def near_rows(b, carry):
        compute(right, b + 2)
        c_near(1, b + 2).start()
        compute(left, b)
        c_near(-1, b).start()
        return carry

    lax.fori_loop(0, 2, near_rows, 0)

    def near_more(b, carry):
        compute(right, b)
        compute(left, b + 2)
        return carry

    lax.fori_loop(0, 2, near_more, 0)

    def add_far(b, carry):
        c_far(1, b, b).wait_recv()
        cbuf[right * NX + b] += far[0, b]
        c_near(1, b).start()
        c_far(-1, b, b + 2).wait_recv()
        cbuf[left * NX + b + 2] += far[1, b]
        c_near(-1, b + 2).start()
        return carry

    lax.fori_loop(0, 2, add_far, 0)

    def own_rows(b, carry):
        compute(x, b)
        return carry

    lax.fori_loop(0, NX, own_rows, 0)

    for b in (0, 2, 1, 3):
        for d in (1, -1):
            c_near(d, b).wait_recv()
        cbuf[x * NX + b] += near[0, b] + near[1, b]
        pltpu.make_async_copy(cbuf.at[x * NX + b], out_hbm.at[pl.ds(b * T, T)], out_sem.at[b]).start()
    p_drain()
    a_drain()
    part = cbuf.at[pl.ds(0, 6)]
    for d in (0, 1):
        pltpu.make_async_copy(part, part, c_send.at[d]).wait()
    for b in range(NX):
        pltpu.make_async_copy(cbuf.at[x * NX + b], out_hbm.at[pl.ds(b * T, T)], out_sem.at[b]).wait()


def body(a_vals, a_cols, a_count, p_vals, p_cols, p_count):
    a = a_vals.reshape(TILES_A, T, T)
    p = p_vals.reshape(TILES_P * T, T)
    hbm = pl.BlockSpec(memory_space=pl.ANY)
    smem = pl.BlockSpec(memory_space=pltpu.SMEM)
    dma = pltpu.SemaphoreType.DMA
    return pl.pallas_call(
        kernel,
        out_shape=jax.ShapeDtypeStruct((NX * T, 2 * T), F32),
        in_specs=[hbm, smem, smem, hbm, smem, smem],
        out_specs=hbm,
        scratch_shapes=[
            pltpu.VMEM((NY * NC, TILES_A, T, T), F32),
            pltpu.VMEM((NY * NC, 8, T), jnp.int32),
            pltpu.SMEM((NY * NC, 8, T), jnp.int32),
            pltpu.VMEM((NZ, PROWS, T), F32),
            pltpu.VMEM((NZ * TILES_P + 1, T, 2 * T), BF),
            pltpu.VMEM((NZ * TILES_P + 1, T, 2 * T), BF),
            pltpu.VMEM((NX * NX, T, 2 * T), F32),
            pltpu.VMEM((2, 2, T, 2 * T), F32),
            pltpu.VMEM((2, NX, T, 2 * T), F32),
            dma((2,)),
            dma((2, 2)),
            dma((2, HALF, TILES_P)),
            dma((2, 2)),
            dma((2, 2, UNITS)),
            dma((3,)),
            dma((3,)),
            dma((2,)),
            dma((4, UNITS)),
            dma((4,)),
            dma((2,)),
            dma((2, 2)),
            dma((2, NX)),
            dma((NX,)),
            dma,
            pltpu.SemaphoreType.REGULAR,
        ],
        compiler_params=pltpu.CompilerParams(collective_id=0, has_side_effects=True, vmem_limit_bytes=60 * 1024 * 1024),
    )(a, a_cols, a_count, p, p_cols, p_count)


def solution(mesh):
    placed = (
        P("gy", "gx", "gz", None, None, None),
        P("gy", "gx", "gz", None),
        P("gy", "gx", "gz"),
        P("gz", "gy", "gx", None, None, None),
        P("gz", "gy", "gx", None),
        P("gz", "gy", "gx"),
    )
    return jax.shard_map(body, mesh=mesh, in_specs=placed, out_specs=P(("gy", "gz"), "gx"), check_vma=False)
```

```python
import jax
import jax.numpy as jnp
from jax import lax
from jax.experimental import pallas as pl
from jax.experimental.pallas import tpu as pltpu
from jax.sharding import PartitionSpec as P

MESH = pl.DeviceIdType.MESH
T = 128
NY = 4
NC = 2
NZ = 16
NX = 4
SLOTS = 6
ROWS_DEV = 2
TILES_A = ROWS_DEV * SLOTS
UNIT = TILES_A // 2
TILES_P = 4
PROWS = TILES_P * T
HALF = NZ // 2
NP = 8
PIECE = TILES_P * T // NP
PLAN0 = ("P0", "A0", "M", 1, 2, 3, "go", 4, 5, "A1", 6, 7, "A2", 8, "A3")
PLAN1 = ("A0", "M", "wait", "P0", 1, 2, "A1", 3, 4, "A2", 5, 6, "A3", 7, 8)
BF = jnp.bfloat16
F32 = jnp.float32


def kernel(
    a_hbm, ac_hbm, an_hbm, p_hbm, pc_hbm, pn_hbm, out,
    abuf, ameta, ameta_s, ac, an, pc, pn, pbuf, pmeta, phi, plo, cbuf, far, near,
    own_sem, p_send, p_recv, pm_send, pm_recv, a_send, a_recv, m_send, m_recv,
    sib_send, sib_recv, smeta_recv, c_send, far_recv, near_recv, out_sem, int_sem, meta_sem, go_sem,
):
    gx, me, x = lax.axis_index("gx"), lax.axis_index("gy"), lax.axis_index("gz")
    y, core = gx // NC, gx % NC

    def wrap(value, n):
        return lax.rem(value + 2 * n, n)

    def y_dev(d):
        return {"gx": wrap(y + d, NY) * NC + core}

    def y_slot(d):
        return wrap(y + d, NY) * NC + core

    sibling = {"gx": y * NC + 1 - core}

    def sib_slot(d):
        return wrap(y + d, NY) * NC + 1 - core

    def remote(src, dst, send, recv, device):
        return pltpu.make_async_remote_copy(
            src_ref=src, dst_ref=dst, send_sem=send, recv_sem=recv, device_id=device, device_id_type=MESH
        )

    own_a = pltpu.make_async_copy(a_hbm, abuf.at[gx], own_sem.at[0])
    own_p = pltpu.make_async_copy(p_hbm, pbuf.at[me], own_sem.at[1])
    own_p.start()
    own_a.start()
    ints = [
        pltpu.make_async_copy(src, dst, int_sem.at[i])
        for i, (src, dst) in enumerate(((ac_hbm, ac), (an_hbm, an), (pc_hbm, pc), (pn_hbm, pn)))
    ]
    for copy in ints:
        copy.start()

    barrier = pltpu.get_barrier_semaphore()
    peers = [sibling, y_dev(1), y_dev(-1), {"gy": wrap(me + 1, NZ)}, {"gy": wrap(me - 1, NZ)}, {"gz": wrap(x + 1, NX)}, {"gz": wrap(x - 1, NX)}]
    for peer in peers:
        pl.semaphore_signal(barrier, inc=1, device_id=peer, device_id_type=MESH)

    pl.semaphore_wait(barrier, len(peers))

    DIR = {1: 0, -1: 1}
    EARLY = {1: 0, -1: 1}

    def a_part(slot, u):
        return abuf.at[slot, pl.ds(u * UNIT, UNIT)]

    def a_first(d, u, slot):
        return remote(a_part(slot, u), a_part(slot, u), a_send.at[DIR[d]], a_recv.at[DIR[d], u], y_dev(d))

    def a_second(d, slot):
        part = a_part(slot, EARLY[d])
        return remote(part, part, a_send.at[DIR[d]], a_recv.at[DIR[d], 2], y_dev(d))

    def m_copy(hop, d, slot):
        return remote(ameta.at[slot], ameta.at[slot], m_send, m_recv.at[hop], y_dev(d))

    def to_sibling(kind, slot, u=None):
        part = abuf.at[slot] if u is None else a_part(slot, u)
        return remote(part, part, sib_send, sib_recv.at[kind], sibling)

    def m_sibling(kind, slot):
        return remote(ameta.at[slot], ameta.at[slot], m_send, smeta_recv.at[kind], sibling)

    def a_start():
        own_a.wait()
        for i in range(2):
            for d in (1, -1):
                a_first(d, EARLY[d] if i == 0 else 1 - EARLY[d], gx).start()
        to_sibling(0, gx).start()

    def a_near():
        for d in (1, -1):
            a_first(d, EARLY[d], y_slot(-d)).wait_recv()
            a_second(d, y_slot(-d)).start()
        for d in (1, -1):
            m_copy(DIR[d], d, y_slot(-d)).wait_recv()
        m_copy(2, 1, y_slot(-1)).start()
        for d in (1, -1):
            a_first(d, 1 - EARLY[d], y_slot(-d)).wait_recv()
            to_sibling(1 + DIR[d], y_slot(-d)).start()
            m_sibling(1 + DIR[d], y_slot(-d)).start()

    def a_far():
        slot = y_slot(2)
        m_copy(2, 1, slot).wait_recv()
        m_sibling(3, slot).start()
        for d in (1, -1):
            a_second(d, slot).wait_recv()
        to_sibling(3, slot).start()

    def a_finish():
        for kind, d in ((0, 0), (1, -1), (2, 1), (3, 2)):
            m_sibling(kind, sib_slot(d)).wait_recv()
            to_sibling(kind, sib_slot(d)).wait_recv()
        copy = pltpu.make_async_copy(ameta, ameta_s, meta_sem)
        copy.start()
        copy.wait()

    def a_drain():
        for d in (0, 1):
            part = abuf.at[pl.ds(0, 3), pl.ds(0, UNIT)]
            pltpu.make_async_copy(part, part, a_send.at[d]).wait()
        part = abuf.at[pl.ds(0, NY)]
        pltpu.make_async_copy(part, part, sib_send).wait()
        part = ameta.at[pl.ds(0, 3 + NY)]
        pltpu.make_async_copy(part, part, m_send).wait()

    PIECES = tuple(range(NP))[::-1]
    LAST = {1: tuple(range(NP // 2)), -1: tuple(range(NP // 2, NP))[::-1]}

    def p_part(slot, j):
        return pbuf.at[slot, pl.ds(j * PIECE, PIECE)]

    def p_copy(d, step, j, slot):
        part = p_part(slot, j)
        return remote(
            part, part, p_send.at[DIR[d]], p_recv.at[DIR[d], step - 1, j], {"gy": wrap(me + d, NZ)}
        )

    def pm_copy(d, step, slot):
        part = pmeta.at[slot]
        return remote(part, part, pm_send.at[DIR[d]], pm_recv.at[DIR[d], step - 1], {"gy": wrap(me + d, NZ)})

    lane = lax.broadcasted_iota(jnp.int32, (TILES_P, T), 1)

    def convert(slot, t):
        p = pbuf[slot, t * T : (t + 1) * T, :]
        packed = pmeta[slot]
        turned = pltpu.roll(packed, T // 2, 1)
        low_half = lane < T // 2
        weights = (jnp.where(low_half, packed, turned), jnp.where(low_half, turned, packed))
        hi = p.astype(BF)
        lo = (p - hi.astype(F32)).astype(BF)
        k = slot * TILES_P + t
        for col in range(2):
            weight = weights[col][t : t + 1, :].astype(BF)
            phi[k, :, col * T : (col + 1) * T] = hi * weight
            plo[k, :, col * T : (col + 1) * T] = lo * weight

    def metas():
        for copy in ints:
            copy.wait()
        row4 = lax.broadcasted_iota(jnp.int32, (TILES_P, T), 0)
        weights = jnp.zeros((TILES_P, T), F32)
        for t in range(TILES_P):
            column = jnp.where(pn[0, t] > 0, pc[0, t], -1)
            named = jnp.where(lane < T // 2, 0, 1) == column
            weights = jnp.where(jnp.logical_and(row4 == t, named), 1.0, weights)
        pmeta[me] = weights
        lane8 = lax.broadcasted_iota(jnp.int32, (8, T), 1)
        targets = jnp.zeros((8, T), jnp.int32)
        for r in range(ROWS_DEV):
            for s in range(SLOTS):
                target = jnp.where(s < an[0, r], ac[0, r, 0, s], NZ * TILES_P)
                targets = jnp.where(lane8 == r * SLOTS + s, target, targets)
        ameta[gx] = targets
        phi[NZ * TILES_P] = jnp.zeros((T, 2 * T), BF)
        plo[NZ * TILES_P] = jnp.zeros((T, 2 * T), BF)
        for d in (1, -1):
            pm_copy(d, 1, me).start()
            m_copy(DIR[d], d, gx).start()
        m_sibling(0, gx).start()

    def p_start():
        own_p.wait()
        for j in PIECES:
            for d in (1, -1):
                p_copy(d, 1, j, me).start()

    PER = NP // TILES_P

    def p_steps(first, last):
        def step(s, carry):
            for i, j in enumerate(PIECES):
                for d in (1, -1):
                    slot = wrap(me - d * s, NZ)
                    p_copy(d, s, j, slot).wait_recv()
                    p_copy(d, s + 1, j, slot).start()
                if i % PER == 0:
                    for d in (1, -1):
                        convert(wrap(me - d * (s - 1), NZ), i // PER)
            for d in (1, -1):
                slot = wrap(me - d * s, NZ)
                pm_copy(d, s, slot).wait_recv()
                pm_copy(d, s + 1, slot).start()
            return carry

        lax.fori_loop(first, last + 1, step, 0)

    def p_seven():
        s = HALF - 1
        for i, j in enumerate(PIECES):
            for d in (1, -1):
                slot = wrap(me - d * s, NZ)
                p_copy(d, s, j, slot).wait_recv()
                if j in LAST[d]:
                    p_copy(d, HALF, j, slot).start()
            if i % PER == 0:
                for d in (1, -1):
                    convert(wrap(me - d * (s - 1), NZ), i // PER)
        for d in (1, -1):
            slot = wrap(me - d * s, NZ)
            pm_copy(d, s, slot).wait_recv()
            if d == -1:
                pm_copy(d, HALF, slot).start()
        for t in range(TILES_P):
            for d in (1, -1):
                convert(wrap(me - d * s, NZ), t)

    def p_eight():
        slot = wrap(me + HALF, NZ)
        pm_copy(-1, HALF, slot).wait_recv()
        for i in range(NP // 2):
            for d in (1, -1):
                p_copy(d, HALF, LAST[d][i], slot).wait_recv()
            if i % PER == PER - 1:
                for d in (1, -1):
                    convert(slot, LAST[d][i] // PER)

    def p_drain():
        part = pbuf.at[pl.ds(0, 2 * HALF - 1), pl.ds(0, 2 * T)]
        for d in (1, -1):
            pltpu.make_async_copy(part, part, p_send.at[DIR[d]]).wait()
            metas_sent = pmeta.at[pl.ds(0, HALF - 1 if d == 1 else HALF)]
            pltpu.make_async_copy(metas_sent, metas_sent, pm_send.at[DIR[d]]).wait()

    def go():
        pl.semaphore_signal(go_sem, inc=1, device_id=sibling, device_id_type=MESH)

    def follow(plan):
        acts = {
            "P0": p_start, "A0": a_start, "A1": a_near, "A2": a_far, "A3": a_finish, "M": metas,
            "go": go, "wait": lambda: pl.semaphore_wait(go_sem, 1),
            HALF - 1: p_seven, HALF: p_eight,
        }
        run = []
        for item in plan + (None,):
            if item in range(1, HALF - 1):
                run.append(item)
                continue
            if run:
                p_steps(run[0], run[-1])
                run = []
            if item is not None:
                acts[item]()

    @pl.when(core == 0)
    def _():
        follow(PLAN0)

    @pl.when(core == 1)
    def _():
        follow(PLAN1)

    def compute(o, b):
        row = o * NX + b
        slot, r = row // ROWS_DEV, row % ROWS_DEV
        total = jnp.zeros((T, 2 * T), F32)
        for pair in range(SLOTS // 2):
            left, high, low = [], [], []
            for s in (2 * pair, 2 * pair + 1):
                k = ameta_s[slot, 0, r * SLOTS + s]
                left.append(abuf[slot, r * SLOTS + s])
                high.append(phi[k])
                low.append(plo[k])
            a = jnp.concatenate(left, axis=1)
            hi = a.astype(BF)
            lo = (a - hi.astype(F32)).astype(BF)
            high = jnp.concatenate(high, axis=0)
            low = jnp.concatenate(low, axis=0)
            total += jnp.dot(hi, high, preferred_element_type=F32)
            total += jnp.dot(lo, high, preferred_element_type=F32)
            total += jnp.dot(hi, low, preferred_element_type=F32)
        cbuf[row] = total

    def c_far(d, h, b):
        return remote(cbuf.at[wrap(x + 2, NX) * NX + b], far.at[DIR[d], h], c_send.at[DIR[d]], far_recv.at[DIR[d], h], {"gz": wrap(x + d, NX)})

    def c_near(d, b):
        return remote(cbuf.at[wrap(x + d, NX) * NX + b], near.at[DIR[d], b], c_send.at[DIR[d]], near_recv.at[DIR[d], b], {"gz": wrap(x + d, NX)})

    opposite, right, left = wrap(x + 2, NX), wrap(x + 1, NX), wrap(x - 1, NX)

    def far_rows(b, carry):
        compute(opposite, b)
        compute(opposite, b + 2)
        c_far(1, b, b).start()
        c_far(-1, b, b + 2).start()
        return carry

    lax.fori_loop(0, 2, far_rows, 0)

    def near_rows(b, carry):
        compute(right, b + 2)
        compute(left, b)
        c_near(1, b + 2).start()
        c_near(-1, b).start()
        return carry

    lax.fori_loop(0, 2, near_rows, 0)

    def near_more(b, carry):
        compute(right, b)
        compute(left, b + 2)
        return carry

    lax.fori_loop(0, 2, near_more, 0)

    def add_far(b, carry):
        c_far(1, b, b).wait_recv()
        cbuf[right * NX + b] += far[0, b]
        c_near(1, b).start()
        c_far(-1, b, b + 2).wait_recv()
        cbuf[left * NX + b + 2] += far[1, b]
        c_near(-1, b + 2).start()
        return carry

    lax.fori_loop(0, 2, add_far, 0)

    def own_rows(b, carry):
        compute(x, b)
        return carry

    lax.fori_loop(0, NX, own_rows, 0)

    def out_copy(b):
        return pltpu.make_async_copy(cbuf.at[x * NX + b], out.at[pl.ds(b * T, T)], out_sem.at[b])

    for b in (0, 2, 1, 3):
        for d in (1, -1):
            c_near(d, b).wait_recv()
        cbuf[x * NX + b] += near[0, b] + near[1, b]
        out_copy(b).start()
    p_drain()
    a_drain()
    part = cbuf.at[pl.ds(0, 6)]
    for d in (0, 1):
        pltpu.make_async_copy(part, part, c_send.at[d]).wait()
    for b in range(NX):
        out_copy(b).wait()


def body(a_vals, a_cols, a_count, p_vals, p_cols, p_count):
    a = a_vals.reshape(TILES_A, T, T)
    p = p_vals.reshape(TILES_P * T, T)
    hbm = pl.BlockSpec(memory_space=pltpu.HBM)
    dma = pltpu.SemaphoreType.DMA
    return pl.pallas_call(
        kernel,
        out_shape=jax.ShapeDtypeStruct((NX * T, 2 * T), F32),
        in_specs=[hbm] * 6,
        out_specs=pl.BlockSpec(memory_space=pl.ANY),
        scratch_shapes=[
            pltpu.VMEM((NY * NC, TILES_A, T, T), F32),
            pltpu.VMEM((NY * NC, 8, T), jnp.int32),
            pltpu.SMEM((NY * NC, 8, T), jnp.int32),
            pltpu.SMEM((1, ROWS_DEV, 1, SLOTS), jnp.int32),
            pltpu.SMEM((1, ROWS_DEV), jnp.int32),
            pltpu.SMEM((1, TILES_P), jnp.int32),
            pltpu.SMEM((1, TILES_P), jnp.int32),
            pltpu.VMEM((NZ, PROWS, T), F32),
            pltpu.VMEM((NZ, TILES_P, T), F32),
            pltpu.VMEM((NZ * TILES_P + 1, T, 2 * T), BF),
            pltpu.VMEM((NZ * TILES_P + 1, T, 2 * T), BF),
            pltpu.VMEM((NX * NX, T, 2 * T), F32),
            pltpu.VMEM((2, 2, T, 2 * T), F32),
            pltpu.VMEM((2, NX, T, 2 * T), F32),
            dma((2,)),
            dma((2,)),
            dma((2, HALF, NP)),
            dma((2,)),
            dma((2, HALF)),
            dma((2,)),
            dma((2, 3)),
            dma,
            dma((3,)),
            dma,
            dma((4,)),
            dma((4,)),
            dma((2,)),
            dma((2, 2)),
            dma((2, NX)),
            dma((NX,)),
            dma((4,)),
            dma,
            pltpu.SemaphoreType.REGULAR,
        ],
        compiler_params=pltpu.CompilerParams(collective_id=0, has_side_effects=True, vmem_limit_bytes=36 * 1024 * 1024),
    )(*(pltpu.with_memory_space_constraint(v, pltpu.HBM) for v in (a, a_cols, a_count.reshape(1, ROWS_DEV), p, p_cols.reshape(1, TILES_P), p_count.reshape(1, TILES_P))))


def solution(mesh):
    placed = (
        P("gy", "gx", "gz", None, None, None),
        P("gy", "gx", "gz", None),
        P("gy", "gx", "gz"),
        P("gz", "gy", "gx", None, None, None),
        P("gz", "gy", "gx", None),
        P("gz", "gy", "gx"),
    )
    return jax.shard_map(body, mesh=mesh, in_specs=placed, out_specs=P(("gy", "gz"), "gx"), check_vma=False)
```

```python
import jax
import jax.numpy as jnp
from jax import lax
from jax.experimental import pallas as pl
from jax.experimental.pallas import tpu as pltpu
from jax.sharding import PartitionSpec as P

MESH = pl.DeviceIdType.MESH
T = 128
NY = 4
NC = 2
NZ = 16
NX = 4
SLOTS = 6
ROWS_DEV = 2
TILES_A = ROWS_DEV * SLOTS
UNIT = TILES_A // 2
TILES_P = 4
PROWS = TILES_P * T
HALF = NZ // 2
NP = 8
DEPTH = 4
PIECE = TILES_P * T // NP
PLAN0 = ("P", "A0", "M", 1, "go", 2, "go", 3, 4, "go", 5, "A1", 6, 7, "A2", 8, "A3")
PLAN1 = ("A0", "M", "Pa", "Pb", "Pc", "A1", 1, 2, "A2", 3, 4, 5, "A3", 6, 7, 8)
BF = jnp.bfloat16
F32 = jnp.float32


def kernel(
    a_hbm, ac_hbm, an_hbm, p_hbm, pc_hbm, pn_hbm, out,
    abuf, ameta, ameta_s, ac, an, pc, pn, pbuf, pmeta, phi, plo, cbuf, far, near,
    own_sem, p_send, p_recv, pm_send, pm_recv, a_send, a_recv, m_send, m_recv,
    sib_send, sib_recv, smeta_recv, c_send, far_recv, near_recv, out_sem, int_sem, meta_sem, go_sem, credit,
):
    gx, me, x = lax.axis_index("gx"), lax.axis_index("gy"), lax.axis_index("gz")
    y, core = gx // NC, gx % NC

    def wrap(value, n):
        return lax.rem(value + 2 * n, n)

    def y_dev(d):
        return {"gx": wrap(y + d, NY) * NC + core}

    def y_slot(d):
        return wrap(y + d, NY) * NC + core

    sibling = {"gx": y * NC + 1 - core}

    def remote(src, dst, send, recv, device):
        return pltpu.make_async_remote_copy(
            src_ref=src, dst_ref=dst, send_sem=send, recv_sem=recv, device_id=device, device_id_type=MESH
        )

    barrier = pltpu.get_barrier_semaphore()
    peers = [sibling, y_dev(1), y_dev(-1), {"gy": wrap(me + 1, NZ)}, {"gy": wrap(me - 1, NZ)}, {"gz": wrap(x + 1, NX)}, {"gz": wrap(x - 1, NX)}]
    for peer in peers:
        pl.semaphore_signal(barrier, inc=1, device_id=peer, device_id_type=MESH)

    own_a = pltpu.make_async_copy(a_hbm, abuf.at[gx], own_sem.at[0])
    own_p = pltpu.make_async_copy(p_hbm, pbuf.at[me], own_sem.at[1])
    own_p.start()
    own_a.start()
    ints = [
        pltpu.make_async_copy(src, dst, int_sem.at[i])
        for i, (src, dst) in enumerate(((ac_hbm, ac), (an_hbm, an), (pc_hbm, pc), (pn_hbm, pn)))
    ]
    for copy in ints:
        copy.start()

    pl.semaphore_wait(barrier, len(peers))

    DIR = {1: 0, -1: 1}
    EARLY = {1: 0, -1: 1}

    def a_part(slot, u):
        return abuf.at[slot, pl.ds(u * UNIT, UNIT)]

    def a_first(d, u, slot):
        return remote(a_part(slot, u), a_part(slot, u), a_send.at[DIR[d]], a_recv.at[DIR[d], u], y_dev(d))

    def a_second(d, slot):
        part = a_part(slot, EARLY[d])
        return remote(part, part, a_send.at[DIR[d]], a_recv.at[DIR[d], 2], y_dev(d))

    def m_copy(hop, d, slot):
        return remote(ameta.at[slot], ameta.at[slot], m_send, m_recv.at[hop], y_dev(d))

    def to_sibling(slot):
        part = abuf.at[slot]
        return remote(part, part, sib_send, sib_recv, sibling)

    def m_sibling(slot):
        return remote(ameta.at[slot], ameta.at[slot], m_send, smeta_recv, sibling)

    def a_start():
        own_a.wait()
        for i in range(2):
            for d in (1, -1):
                a_first(d, EARLY[d] if i == 0 else 1 - EARLY[d], gx).start()
        to_sibling(gx).start()

    def a_near():
        for d in (1, -1):
            a_first(d, EARLY[d], y_slot(-d)).wait_recv()
            a_second(d, y_slot(-d)).start()
        for d in (1, -1):
            m_copy(DIR[d], d, y_slot(-d)).wait_recv()
        m_copy(2, 1, y_slot(-1)).start()
        for d in (1, -1):
            a_first(d, 1 - EARLY[d], y_slot(-d)).wait_recv()
            to_sibling(y_slot(-d)).start()
            m_sibling(y_slot(-d)).start()

    def a_far():
        slot = y_slot(2)
        m_copy(2, 1, slot).wait_recv()
        m_sibling(slot).start()
        for d in (1, -1):
            a_second(d, slot).wait_recv()
        to_sibling(slot).start()

    to_smem = pltpu.make_async_copy(ameta, ameta_s, meta_sem)

    def a_finish():
        part = ameta.at[pl.ds(0, NY)]
        pltpu.make_async_copy(part, part, smeta_recv).wait()
        part = abuf.at[pl.ds(0, NY)]
        pltpu.make_async_copy(part, part, sib_recv).wait()
        to_smem.start()

    def a_drain():
        for d in (0, 1):
            part = abuf.at[pl.ds(0, 3), pl.ds(0, UNIT)]
            pltpu.make_async_copy(part, part, a_send.at[d]).wait()
        part = abuf.at[pl.ds(0, NY)]
        pltpu.make_async_copy(part, part, sib_send).wait()
        part = ameta.at[pl.ds(0, 3 + NY)]
        pltpu.make_async_copy(part, part, m_send).wait()

    PIECES = tuple(range(NP))[::-1]
    LAST = {1: tuple(range(NP // 2)), -1: tuple(range(NP // 2, NP))[::-1]}

    def p_part(slot, j):
        return pbuf.at[slot, pl.ds(j * PIECE, PIECE)]

    def p_copy(d, step, j, slot):
        part = p_part(slot, j)
        return remote(
            part, part, p_send.at[DIR[d]], p_recv.at[DIR[d], (step - 1) % DEPTH, j], {"gy": wrap(me + d, NZ)}
        )

    def pm_copy(d, step, slot):
        part = pmeta.at[slot]
        return remote(part, part, pm_send.at[DIR[d]], pm_recv.at[DIR[d], (step - 1) % DEPTH], {"gy": wrap(me + d, NZ)})

    lane = lax.broadcasted_iota(jnp.int32, (TILES_P, T), 1)

    def convert(slot, t):
        p = pbuf[slot, t * T : (t + 1) * T, :]
        packed = pmeta[slot]
        turned = pltpu.roll(packed, T // 2, 1)
        low_half = lane < T // 2
        weights = (jnp.where(low_half, packed, turned), jnp.where(low_half, turned, packed))
        hi = p.astype(BF)
        lo = (p - hi.astype(F32)).astype(BF)
        k = slot * TILES_P + t
        for col in range(2):
            weight = weights[col][t : t + 1, :].astype(BF)
            phi[k, :, col * T : (col + 1) * T] = hi * weight
            plo[k, :, col * T : (col + 1) * T] = lo * weight

    def metas():
        for copy in ints:
            copy.wait()
        row4 = lax.broadcasted_iota(jnp.int32, (TILES_P, T), 0)
        weights = jnp.zeros((TILES_P, T), F32)
        for t in range(TILES_P):
            column = jnp.where(pn[0, t] > 0, pc[0, t], -1)
            named = jnp.where(lane < T // 2, 0, 1) == column
            weights = jnp.where(jnp.logical_and(row4 == t, named), 1.0, weights)
        pmeta[me] = weights
        lane1 = lax.broadcasted_iota(jnp.int32, (1, T), 1)
        targets = jnp.zeros((1, T), jnp.int32)
        for r in range(ROWS_DEV):
            for s in range(SLOTS):
                target = jnp.where(s < an[0, r], ac[0, r, 0, s], NZ * TILES_P)
                targets = jnp.where(lane1 == r * SLOTS + s, target, targets)
        ameta[gx] = targets
        phi[NZ * TILES_P] = jnp.zeros((T, 2 * T), BF)
        plo[NZ * TILES_P] = jnp.zeros((T, 2 * T), BF)
        for d in (1, -1):
            pm_copy(d, 1, me).start()
            m_copy(DIR[d], d, gx).start()
        m_sibling(gx).start()

    def p_send_own(pieces):
        for j in pieces:
            for d in (1, -1):
                p_copy(d, 1, j, me).start()

    def p_start():
        own_p.wait()
        p_send_own(PIECES)

    def p_begin(first, last):
        def act():
            if first == 0:
                own_p.wait()
            pl.semaphore_wait(go_sem, 1)
            p_send_own(PIECES[first:last])

        return act

    PER = NP // TILES_P

    def spend():
        for d in (1, -1):
            pl.semaphore_wait(credit.at[DIR[d]], 1)

    def give():
        for d in (1, -1):
            pl.semaphore_signal(
                credit.at[DIR[d]], inc=1, device_id={"gy": wrap(me - d, NZ)}, device_id_type=MESH
            )

    def p_steps(first, last):
        def step(s, carry):
            pl.when(s >= DEPTH)(spend)
            for i, j in enumerate(PIECES):
                for d in (1, -1):
                    slot = wrap(me - d * s, NZ)
                    p_copy(d, s, j, slot).wait_recv()
                    p_copy(d, s + 1, j, slot).start()
                if i % PER == 0:
                    for d in (1, -1):
                        convert(wrap(me - d * (s - 1), NZ), i // PER)
            for d in (1, -1):
                slot = wrap(me - d * s, NZ)
                pm_copy(d, s, slot).wait_recv()
                pm_copy(d, s + 1, slot).start()
            pl.when(s <= HALF - DEPTH)(give)
            return carry

        lax.fori_loop(first, last + 1, step, 0)

    def p_seven():
        s = HALF - 1
        spend()
        for i, j in enumerate(PIECES):
            for d in (1, -1):
                slot = wrap(me - d * s, NZ)
                p_copy(d, s, j, slot).wait_recv()
                if j in LAST[d]:
                    p_copy(d, HALF, j, slot).start()
            if i % PER == 0:
                for d in (1, -1):
                    convert(wrap(me - d * (s - 1), NZ), i // PER)
        for d in (1, -1):
            slot = wrap(me - d * s, NZ)
            pm_copy(d, s, slot).wait_recv()
            if d == -1:
                pm_copy(d, HALF, slot).start()
        for t in range(TILES_P):
            for d in (1, -1):
                convert(wrap(me - d * s, NZ), t)

    def p_eight():
        slot = wrap(me + HALF, NZ)
        pm_copy(-1, HALF, slot).wait_recv()
        for i in range(NP // 2):
            for d in (1, -1):
                p_copy(d, HALF, LAST[d][i], slot).wait_recv()
            if i % PER == PER - 1:
                for d in (1, -1):
                    convert(slot, LAST[d][i] // PER)

    def p_drain():
        part = pbuf.at[pl.ds(0, 2 * HALF - 1), pl.ds(0, 2 * T)]
        for d in (1, -1):
            pltpu.make_async_copy(part, part, p_send.at[DIR[d]]).wait()
            metas_sent = pmeta.at[pl.ds(0, HALF - 1 if d == 1 else HALF)]
            pltpu.make_async_copy(metas_sent, metas_sent, pm_send.at[DIR[d]]).wait()

    def go():
        pl.semaphore_signal(go_sem, inc=1, device_id=sibling, device_id_type=MESH)

    def follow(plan):
        acts = {
            "P": p_start, "Pa": p_begin(0, 3), "Pb": p_begin(3, 6), "Pc": p_begin(6, NP), "A0": a_start, "A1": a_near, "A2": a_far, "A3": a_finish, "M": metas,
            "go": go,
            HALF - 1: p_seven, HALF: p_eight,
        }
        run = []
        for item in plan + (None,):
            if item in range(1, HALF - 1):
                run.append(item)
                continue
            if run:
                p_steps(run[0], run[-1])
                run = []
            if item is not None:
                acts[item]()

    @pl.when(core == 0)
    def _():
        follow(PLAN0)

    @pl.when(core == 1)
    def _():
        follow(PLAN1)

    def compute(o, b):
        row = o * NX + b
        slot, r = row // ROWS_DEV, row % ROWS_DEV
        total = jnp.zeros((T, 2 * T), F32)
        for pair in range(SLOTS // 2):
            left, high, low = [], [], []
            for s in (2 * pair, 2 * pair + 1):
                k = ameta_s[slot, 0, r * SLOTS + s]
                left.append(abuf[slot, r * SLOTS + s])
                high.append(phi[k])
                low.append(plo[k])
            a = jnp.concatenate(left, axis=1)
            hi = a.astype(BF)
            lo = (a - hi.astype(F32)).astype(BF)
            high = jnp.concatenate(high, axis=0)
            low = jnp.concatenate(low, axis=0)
            total += jnp.dot(hi, high, preferred_element_type=F32)
            total += jnp.dot(lo, high, preferred_element_type=F32)
            total += jnp.dot(hi, low, preferred_element_type=F32)
        cbuf[row] = total

    def c_far(d, h, b):
        return remote(cbuf.at[wrap(x + 2, NX) * NX + b], far.at[DIR[d], h], c_send.at[DIR[d]], far_recv.at[DIR[d], h], {"gz": wrap(x + d, NX)})

    def c_near(d, b):
        return remote(cbuf.at[wrap(x + d, NX) * NX + b], near.at[DIR[d], b], c_send.at[DIR[d]], near_recv.at[DIR[d], b], {"gz": wrap(x + d, NX)})

    to_smem.wait()
    opposite, right, left = wrap(x + 2, NX), wrap(x + 1, NX), wrap(x - 1, NX)

    def far_rows(b, carry):
        compute(opposite, b)
        compute(opposite, b + 2)
        c_far(1, b, b).start()
        c_far(-1, b, b + 2).start()
        return carry

    lax.fori_loop(0, 2, far_rows, 0)

    def near_rows(b, carry):
        compute(right, b + 2)
        compute(left, b)
        c_near(1, b + 2).start()
        c_near(-1, b).start()
        return carry

    lax.fori_loop(0, 2, near_rows, 0)

    def near_more(b, carry):
        compute(right, b)
        compute(left, b + 2)
        return carry

    lax.fori_loop(0, 2, near_more, 0)

    def add_far(b, carry):
        c_far(1, b, b).wait_recv()
        cbuf[right * NX + b] += far[0, b]
        c_near(1, b).start()
        c_far(-1, b, b + 2).wait_recv()
        cbuf[left * NX + b + 2] += far[1, b]
        c_near(-1, b + 2).start()
        return carry

    lax.fori_loop(0, 2, add_far, 0)

    def own_rows(b, carry):
        compute(x, b)
        return carry

    lax.fori_loop(0, NX, own_rows, 0)

    def out_copy(b):
        return pltpu.make_async_copy(cbuf.at[x * NX + b], out.at[pl.ds(b * T, T)], out_sem)

    for b in (0, 2, 1, 3):
        for d in (1, -1):
            c_near(d, b).wait_recv()
        cbuf[x * NX + b] += near[0, b] + near[1, b]
        out_copy(b).start()
    p_drain()
    a_drain()
    part = cbuf.at[pl.ds(0, 6)]
    for d in (0, 1):
        pltpu.make_async_copy(part, part, c_send.at[d]).wait()
    part = cbuf.at[pl.ds(0, NX)]
    pltpu.make_async_copy(part, part, out_sem).wait()


def body(a_vals, a_cols, a_count, p_vals, p_cols, p_count):
    a = a_vals.reshape(TILES_A, T, T)
    p = p_vals.reshape(TILES_P * T, T)
    hbm = pl.BlockSpec(memory_space=pltpu.HBM)
    dma = pltpu.SemaphoreType.DMA
    return pl.pallas_call(
        kernel,
        out_shape=jax.ShapeDtypeStruct((NX * T, 2 * T), F32),
        in_specs=[hbm] * 6,
        out_specs=pl.BlockSpec(memory_space=pl.ANY),
        scratch_shapes=[
            pltpu.VMEM((NY * NC, TILES_A, T, T), F32),
            pltpu.VMEM((NY * NC, 1, T), jnp.int32),
            pltpu.SMEM((NY * NC, 1, T), jnp.int32),
            pltpu.SMEM((1, ROWS_DEV, 1, SLOTS), jnp.int32),
            pltpu.SMEM((1, ROWS_DEV), jnp.int32),
            pltpu.SMEM((1, TILES_P), jnp.int32),
            pltpu.SMEM((1, TILES_P), jnp.int32),
            pltpu.VMEM((NZ, PROWS, T), F32),
            pltpu.VMEM((NZ, TILES_P, T), F32),
            pltpu.VMEM((NZ * TILES_P + 1, T, 2 * T), BF),
            pltpu.VMEM((NZ * TILES_P + 1, T, 2 * T), BF),
            pltpu.VMEM((NX * NX, T, 2 * T), F32),
            pltpu.VMEM((2, 2, T, 2 * T), F32),
            pltpu.VMEM((2, NX, T, 2 * T), F32),
            dma((2,)),
            dma((2,)),
            dma((2, DEPTH, NP)),
            dma((2,)),
            dma((2, DEPTH)),
            dma((2,)),
            dma((2, 3)),
            dma,
            dma((3,)),
            dma,
            dma,
            dma,
            dma((2,)),
            dma((2, 2)),
            dma((2, NX)),
            dma,
            dma((4,)),
            dma,
            pltpu.SemaphoreType.REGULAR,
            pltpu.SemaphoreType.REGULAR((2,)),
        ],
        compiler_params=pltpu.CompilerParams(collective_id=0, has_side_effects=True, vmem_limit_bytes=36 * 1024 * 1024),
    )(*(pltpu.with_memory_space_constraint(v, pltpu.HBM) for v in (a, a_cols, a_count.reshape(1, ROWS_DEV), p, p_cols.reshape(1, TILES_P), p_count.reshape(1, TILES_P))))


def solution(mesh):
    placed = (
        P("gy", "gx", "gz", None, None, None),
        P("gy", "gx", "gz", None),
        P("gy", "gx", "gz"),
        P("gz", "gy", "gx", None, None, None),
        P("gz", "gy", "gx", None),
        P("gz", "gy", "gx"),
    )
    return jax.shard_map(body, mesh=mesh, in_specs=placed, out_specs=P(("gy", "gz"), "gx"), check_vma=False)
```

```python
import jax
import jax.numpy as jnp
from jax import lax
from jax.experimental import pallas as pl
from jax.experimental.pallas import tpu as pltpu
from jax.sharding import PartitionSpec as P

MESH = pl.DeviceIdType.MESH
T = 128
NY = 4
NC = 2
NZ = 16
NX = 4
SLOTS = 6
ROWS_DEV = 2
TILES_A = ROWS_DEV * SLOTS
UNIT = TILES_A // 2
TILES_P = 4
PROWS = TILES_P * T
HALF = NZ // 2
NP = 8
DEPTH = 4
PIECE = TILES_P * T // NP
PLAN0 = ("P", "A0", "M", 1, "go", 2, 3, "go", 4, 5, "A1", 6, 7, "A2", 8, "A3")
PLAN1 = ("Pa", "A0", "M", "Pb", "Pc", 1, "A1", 2, 3, "A2", 4, 5, "A3", 6, 7, 8)
BF = jnp.bfloat16
F32 = jnp.float32


def kernel(
    a_hbm, ac_hbm, an_hbm, p_hbm, pc_hbm, pn_hbm, out,
    abuf, ameta, ameta_s, ac, an, pc, pn, pbuf, pmeta, phi, plo, cbuf, far, near,
    own_sem, p_send, p_recv, pm_send, pm_recv, a_send, a_recv, m_send, m_recv,
    sib_send, sib_recv, smeta_recv, c_send, far_recv, near_recv, out_sem, int_sem, meta_sem, go_sem, credit,
):
    gx, me, x = lax.axis_index("gx"), lax.axis_index("gy"), lax.axis_index("gz")
    y, core = gx // NC, gx % NC

    def wrap(value, n):
        return lax.rem(value + 2 * n, n)

    def y_dev(d):
        return {"gx": wrap(y + d, NY) * NC + core}

    def y_slot(d):
        return wrap(y + d, NY) * NC + core

    sibling = {"gx": y * NC + 1 - core}

    def remote(src, dst, send, recv, device):
        return pltpu.make_async_remote_copy(
            src_ref=src, dst_ref=dst, send_sem=send, recv_sem=recv, device_id=device, device_id_type=MESH
        )

    barrier = pltpu.get_barrier_semaphore()
    peers = [sibling, y_dev(1), y_dev(-1), {"gy": wrap(me + 1, NZ)}, {"gy": wrap(me - 1, NZ)}, {"gz": wrap(x + 1, NX)}, {"gz": wrap(x - 1, NX)}]
    for peer in peers:
        pl.semaphore_signal(barrier, inc=1, device_id=peer, device_id_type=MESH)

    own_a = pltpu.make_async_copy(a_hbm, abuf.at[gx], own_sem.at[0])
    own_p = pltpu.make_async_copy(p_hbm, pbuf.at[me], own_sem.at[1])
    own_p.start()
    own_a.start()
    ints = [
        pltpu.make_async_copy(src, dst, int_sem.at[i])
        for i, (src, dst) in enumerate(((ac_hbm, ac), (an_hbm, an), (pc_hbm, pc), (pn_hbm, pn)))
    ]
    for copy in ints:
        copy.start()

    pl.semaphore_wait(barrier, len(peers))

    DIR = {1: 0, -1: 1}
    EARLY = {1: 0, -1: 1}

    def a_part(slot, u):
        return abuf.at[slot, pl.ds(u * UNIT, UNIT)]

    def a_first(d, u, slot):
        return remote(a_part(slot, u), a_part(slot, u), a_send.at[DIR[d]], a_recv.at[DIR[d], u], y_dev(d))

    def a_second(d, slot):
        part = a_part(slot, EARLY[d])
        return remote(part, part, a_send.at[DIR[d]], a_recv.at[DIR[d], 2], y_dev(d))

    def m_copy(hop, d, slot):
        return remote(ameta.at[slot], ameta.at[slot], m_send, m_recv.at[hop], y_dev(d))

    def to_sibling(slot):
        part = abuf.at[slot]
        return remote(part, part, sib_send, sib_recv, sibling)

    def m_sibling(slot):
        return remote(ameta.at[slot], ameta.at[slot], m_send, smeta_recv, sibling)

    def a_start():
        own_a.wait()
        for i in range(2):
            for d in (1, -1):
                a_first(d, EARLY[d] if i == 0 else 1 - EARLY[d], gx).start()
        to_sibling(gx).start()

    def a_near():
        for d in (1, -1):
            a_first(d, EARLY[d], y_slot(-d)).wait_recv()
            a_second(d, y_slot(-d)).start()
        for d in (1, -1):
            m_copy(DIR[d], d, y_slot(-d)).wait_recv()
        m_copy(2, 1, y_slot(-1)).start()
        for d in (1, -1):
            a_first(d, 1 - EARLY[d], y_slot(-d)).wait_recv()
            to_sibling(y_slot(-d)).start()
            m_sibling(y_slot(-d)).start()

    def a_far():
        slot = y_slot(2)
        m_copy(2, 1, slot).wait_recv()
        m_sibling(slot).start()
        for d in (1, -1):
            a_second(d, slot).wait_recv()
        to_sibling(slot).start()

    to_smem = pltpu.make_async_copy(ameta, ameta_s, meta_sem)

    def a_finish():
        part = ameta.at[pl.ds(0, NY)]
        pltpu.make_async_copy(part, part, smeta_recv).wait()
        part = abuf.at[pl.ds(0, NY)]
        pltpu.make_async_copy(part, part, sib_recv).wait()
        to_smem.start()

    def a_drain():
        for d in (0, 1):
            part = abuf.at[pl.ds(0, 3), pl.ds(0, UNIT)]
            pltpu.make_async_copy(part, part, a_send.at[d]).wait()
        part = abuf.at[pl.ds(0, NY)]
        pltpu.make_async_copy(part, part, sib_send).wait()
        part = ameta.at[pl.ds(0, 3 + NY)]
        pltpu.make_async_copy(part, part, m_send).wait()

    PIECES = tuple(range(NP))[::-1]
    LAST = {1: tuple(range(NP // 2)), -1: tuple(range(NP // 2, NP))[::-1]}

    def p_part(slot, j):
        return pbuf.at[slot, pl.ds(j * PIECE, PIECE)]

    def p_copy(d, step, j, slot):
        part = p_part(slot, j)
        return remote(
            part, part, p_send.at[DIR[d]], p_recv.at[DIR[d], (step - 1) % DEPTH, j], {"gy": wrap(me + d, NZ)}
        )

    def pm_copy(d, step, slot):
        part = pmeta.at[slot]
        return remote(part, part, pm_send.at[DIR[d]], pm_recv.at[DIR[d], (step - 1) % DEPTH], {"gy": wrap(me + d, NZ)})

    lane = lax.broadcasted_iota(jnp.int32, (TILES_P, T), 1)

    def convert(slot, t):
        p = pbuf[slot, t * T : (t + 1) * T, :]
        packed = pmeta[slot]
        turned = pltpu.roll(packed, T // 2, 1)
        low_half = lane < T // 2
        weights = (jnp.where(low_half, packed, turned), jnp.where(low_half, turned, packed))
        hi = p.astype(BF)
        lo = (p - hi.astype(F32)).astype(BF)
        k = slot * TILES_P + t
        for col in range(2):
            weight = weights[col][t : t + 1, :].astype(BF)
            phi[k, :, col * T : (col + 1) * T] = hi * weight
            plo[k, :, col * T : (col + 1) * T] = lo * weight

    def metas():
        for copy in ints:
            copy.wait()
        row4 = lax.broadcasted_iota(jnp.int32, (TILES_P, T), 0)
        weights = jnp.zeros((TILES_P, T), F32)
        for t in range(TILES_P):
            column = jnp.where(pn[0, t] > 0, pc[0, t], -1)
            named = jnp.where(lane < T // 2, 0, 1) == column
            weights = jnp.where(jnp.logical_and(row4 == t, named), 1.0, weights)
        pmeta[me] = weights
        lane1 = lax.broadcasted_iota(jnp.int32, (1, T), 1)
        targets = jnp.zeros((1, T), jnp.int32)
        for r in range(ROWS_DEV):
            for s in range(SLOTS):
                target = jnp.where(s < an[0, r], ac[0, r, 0, s], NZ * TILES_P)
                targets = jnp.where(lane1 == r * SLOTS + s, target, targets)
        ameta[gx] = targets
        phi[NZ * TILES_P] = jnp.zeros((T, 2 * T), BF)
        plo[NZ * TILES_P] = jnp.zeros((T, 2 * T), BF)
        for d in (1, -1):
            pm_copy(d, 1, me).start()
            m_copy(DIR[d], d, gx).start()
        m_sibling(gx).start()

    def p_send_own(pieces):
        for j in pieces:
            for d in (1, -1):
                p_copy(d, 1, j, me).start()

    def p_start():
        own_p.wait()
        p_send_own(PIECES)

    def p_begin(first, last, held=True):
        def act():
            if first == 0:
                own_p.wait()
            if held:
                pl.semaphore_wait(go_sem, 1)
            p_send_own(PIECES[first:last])

        return act

    PER = NP // TILES_P

    def spend():
        for d in (1, -1):
            pl.semaphore_wait(credit.at[DIR[d]], 1)

    def give():
        for d in (1, -1):
            pl.semaphore_signal(
                credit.at[DIR[d]], inc=1, device_id={"gy": wrap(me - d, NZ)}, device_id_type=MESH
            )

    def p_steps(first, last):
        def step(s, carry):
            pl.when(s >= DEPTH)(spend)
            for i, j in enumerate(PIECES):
                for d in (1, -1):
                    slot = wrap(me - d * s, NZ)
                    p_copy(d, s, j, slot).wait_recv()
                    p_copy(d, s + 1, j, slot).start()
                if i % PER == 0:
                    for d in (1, -1):
                        convert(wrap(me - d * (s - 1), NZ), i // PER)
            for d in (1, -1):
                slot = wrap(me - d * s, NZ)
                pm_copy(d, s, slot).wait_recv()
                pm_copy(d, s + 1, slot).start()
            pl.when(s <= HALF - DEPTH)(give)
            return carry

        lax.fori_loop(first, last + 1, step, 0)

    def p_seven():
        s = HALF - 1
        spend()
        for i, j in enumerate(PIECES):
            for d in (1, -1):
                slot = wrap(me - d * s, NZ)
                p_copy(d, s, j, slot).wait_recv()
                if j in LAST[d]:
                    p_copy(d, HALF, j, slot).start()
            if i % PER == 0:
                for d in (1, -1):
                    convert(wrap(me - d * (s - 1), NZ), i // PER)
        for d in (1, -1):
            slot = wrap(me - d * s, NZ)
            pm_copy(d, s, slot).wait_recv()
            if d == -1:
                pm_copy(d, HALF, slot).start()
        for t in range(TILES_P):
            for d in (1, -1):
                convert(wrap(me - d * s, NZ), t)

    def p_eight():
        slot = wrap(me + HALF, NZ)
        pm_copy(-1, HALF, slot).wait_recv()
        for i in range(NP // 2):
            for d in (1, -1):
                p_copy(d, HALF, LAST[d][i], slot).wait_recv()
            if i % PER == PER - 1:
                for d in (1, -1):
                    convert(slot, LAST[d][i] // PER)

    def p_drain():
        part = pbuf.at[pl.ds(0, 2 * HALF - 1), pl.ds(0, 2 * T)]
        for d in (1, -1):
            pltpu.make_async_copy(part, part, p_send.at[DIR[d]]).wait()
            metas_sent = pmeta.at[pl.ds(0, HALF - 1 if d == 1 else HALF)]
            pltpu.make_async_copy(metas_sent, metas_sent, pm_send.at[DIR[d]]).wait()

    def go():
        pl.semaphore_signal(go_sem, inc=1, device_id=sibling, device_id_type=MESH)

    def follow(plan):
        acts = {
            "P": p_start, "Pa": p_begin(0, 3, False), "Pb": p_begin(3, 6), "Pc": p_begin(6, NP), "A0": a_start, "A1": a_near, "A2": a_far, "A3": a_finish, "M": metas,
            "go": go,
            HALF - 1: p_seven, HALF: p_eight,
        }
        run = []
        for item in plan + (None,):
            if item in range(1, HALF - 1):
                run.append(item)
                continue
            if run:
                p_steps(run[0], run[-1])
                run = []
            if item is not None:
                acts[item]()

    @pl.when(core == 0)
    def _():
        follow(PLAN0)

    @pl.when(core == 1)
    def _():
        follow(PLAN1)

    def compute(o, b):
        row = o * NX + b
        slot, r = row // ROWS_DEV, row % ROWS_DEV
        total = jnp.zeros((T, 2 * T), F32)
        for pair in range(SLOTS // 2):
            left, high, low = [], [], []
            for s in (2 * pair, 2 * pair + 1):
                k = ameta_s[slot, 0, r * SLOTS + s]
                left.append(abuf[slot, r * SLOTS + s])
                high.append(phi[k])
                low.append(plo[k])
            a = jnp.concatenate(left, axis=1)
            hi = a.astype(BF)
            lo = (a - hi.astype(F32)).astype(BF)
            high = jnp.concatenate(high, axis=0)
            low = jnp.concatenate(low, axis=0)
            total += jnp.dot(hi, high, preferred_element_type=F32)
            total += jnp.dot(lo, high, preferred_element_type=F32)
            total += jnp.dot(hi, low, preferred_element_type=F32)
        cbuf[row] = total

    def c_far(d, h, b):
        return remote(cbuf.at[wrap(x + 2, NX) * NX + b], far.at[DIR[d], h], c_send.at[DIR[d]], far_recv.at[DIR[d], h], {"gz": wrap(x + d, NX)})

    def c_near(d, b):
        return remote(cbuf.at[wrap(x + d, NX) * NX + b], near.at[DIR[d], b], c_send.at[DIR[d]], near_recv.at[DIR[d], b], {"gz": wrap(x + d, NX)})

    to_smem.wait()
    opposite, right, left = wrap(x + 2, NX), wrap(x + 1, NX), wrap(x - 1, NX)

    def far_rows(b, carry):
        compute(opposite, b)
        compute(opposite, b + 2)
        c_far(1, b, b).start()
        c_far(-1, b, b + 2).start()
        return carry

    lax.fori_loop(0, 2, far_rows, 0)

    def near_rows(b, carry):
        compute(right, b + 2)
        compute(left, b)
        c_near(1, b + 2).start()
        c_near(-1, b).start()
        return carry

    lax.fori_loop(0, 2, near_rows, 0)

    def near_more(b, carry):
        compute(right, b)
        compute(left, b + 2)
        return carry

    lax.fori_loop(0, 2, near_more, 0)

    def add_far(b, carry):
        c_far(1, b, b).wait_recv()
        cbuf[right * NX + b] += far[0, b]
        c_near(1, b).start()
        c_far(-1, b, b + 2).wait_recv()
        cbuf[left * NX + b + 2] += far[1, b]
        c_near(-1, b + 2).start()
        return carry

    lax.fori_loop(0, 2, add_far, 0)

    def own_rows(b, carry):
        compute(x, b)
        return carry

    lax.fori_loop(0, NX, own_rows, 0)

    def out_copy(b):
        return pltpu.make_async_copy(cbuf.at[x * NX + b], out.at[pl.ds(b * T, T)], out_sem)

    for b in (0, 2, 1, 3):
        for d in (1, -1):
            c_near(d, b).wait_recv()
        cbuf[x * NX + b] += near[0, b] + near[1, b]
        out_copy(b).start()
    p_drain()
    a_drain()
    part = cbuf.at[pl.ds(0, 6)]
    for d in (0, 1):
        pltpu.make_async_copy(part, part, c_send.at[d]).wait()
    part = cbuf.at[pl.ds(0, NX)]
    pltpu.make_async_copy(part, part, out_sem).wait()


def body(a_vals, a_cols, a_count, p_vals, p_cols, p_count):
    a = a_vals.reshape(TILES_A, T, T)
    p = p_vals.reshape(TILES_P * T, T)
    hbm = pl.BlockSpec(memory_space=pltpu.HBM)
    dma = pltpu.SemaphoreType.DMA
    return pl.pallas_call(
        kernel,
        out_shape=jax.ShapeDtypeStruct((NX * T, 2 * T), F32),
        in_specs=[hbm] * 6,
        out_specs=pl.BlockSpec(memory_space=pl.ANY),
        scratch_shapes=[
            pltpu.VMEM((NY * NC, TILES_A, T, T), F32),
            pltpu.VMEM((NY * NC, 1, T), jnp.int32),
            pltpu.SMEM((NY * NC, 1, T), jnp.int32),
            pltpu.SMEM((1, ROWS_DEV, 1, SLOTS), jnp.int32),
            pltpu.SMEM((1, ROWS_DEV), jnp.int32),
            pltpu.SMEM((1, TILES_P), jnp.int32),
            pltpu.SMEM((1, TILES_P), jnp.int32),
            pltpu.VMEM((NZ, PROWS, T), F32),
            pltpu.VMEM((NZ, TILES_P, T), F32),
            pltpu.VMEM((NZ * TILES_P + 1, T, 2 * T), BF),
            pltpu.VMEM((NZ * TILES_P + 1, T, 2 * T), BF),
            pltpu.VMEM((NX * NX, T, 2 * T), F32),
            pltpu.VMEM((2, 2, T, 2 * T), F32),
            pltpu.VMEM((2, NX, T, 2 * T), F32),
            dma((2,)),
            dma((2,)),
            dma((2, DEPTH, NP)),
            dma((2,)),
            dma((2, DEPTH)),
            dma((2,)),
            dma((2, 3)),
            dma,
            dma((3,)),
            dma,
            dma,
            dma,
            dma((2,)),
            dma((2, 2)),
            dma((2, NX)),
            dma,
            dma((4,)),
            dma,
            pltpu.SemaphoreType.REGULAR,
            pltpu.SemaphoreType.REGULAR((2,)),
        ],
        compiler_params=pltpu.CompilerParams(collective_id=0, has_side_effects=True, vmem_limit_bytes=36 * 1024 * 1024),
    )(*(pltpu.with_memory_space_constraint(v, pltpu.HBM) for v in (a, a_cols, a_count.reshape(1, ROWS_DEV), p, p_cols.reshape(1, TILES_P), p_count.reshape(1, TILES_P))))


def solution(mesh):
    placed = (
        P("gy", "gx", "gz", None, None, None),
        P("gy", "gx", "gz", None),
        P("gy", "gx", "gz"),
        P("gz", "gy", "gx", None, None, None),
        P("gz", "gy", "gx", None),
        P("gz", "gy", "gx"),
    )
    return jax.shard_map(body, mesh=mesh, in_specs=placed, out_specs=P(("gy", "gz"), "gx"), check_vma=False)
```

```python
import jax
import jax.numpy as jnp
from jax import lax
from jax.experimental import pallas as pl
from jax.experimental.pallas import tpu as pltpu
from jax.sharding import PartitionSpec as P

MESH = pl.DeviceIdType.MESH
T = 128
NY = 4
NC = 2
NZ = 16
NX = 4
SLOTS = 6
ROWS_DEV = 2
TILES_A = ROWS_DEV * SLOTS
UNIT = TILES_A // 2
TILES_P = 4
PROWS = TILES_P * T
HALF = NZ // 2
NP = 8
DEPTH = 4
PIECE = TILES_P * T // NP
PLAN0 = ("P", "A0", "M", 1, "go", 2, 3, "go", 4, 5, "A1", 6, 7, "A2", 8, "A3")
PLAN1 = ("Pa", "A0", "M", "Pb", "Pc", 1, "A1", 2, 3, "A2", 4, 5, "A3", 6, 7, 8)
BF = jnp.bfloat16
F32 = jnp.float32


def kernel(
    a_hbm, ac_hbm, an_hbm, p_hbm, pc_hbm, pn_hbm, out,
    abuf, ameta, ameta_s, ac, an, pc, pn, pbuf, pmeta, phi, plo, cbuf, far, near,
    own_sem, p_send, p_recv, pm_send, pm_recv, a_send, a_recv, m_send, m_recv,
    sib_send, sib_recv, smeta_recv, c_send, far_recv, near_recv, out_sem, int_sem, meta_sem, go_sem, credit,
):
    gx, me, x = lax.axis_index("gx"), lax.axis_index("gy"), lax.axis_index("gz")
    y, core = gx // NC, gx % NC

    def wrap(value, n):
        return lax.rem(value + 2 * n, n)

    def y_dev(d):
        return {"gx": wrap(y + d, NY) * NC + core}

    def y_slot(d):
        return wrap(y + d, NY) * NC + core

    sibling = {"gx": y * NC + 1 - core}

    def remote(src, dst, send, recv, device):
        return pltpu.make_async_remote_copy(
            src_ref=src, dst_ref=dst, send_sem=send, recv_sem=recv, device_id=device, device_id_type=MESH
        )

    barrier = pltpu.get_barrier_semaphore()
    peers = [sibling, y_dev(1), y_dev(-1), {"gy": wrap(me + 1, NZ)}, {"gy": wrap(me - 1, NZ)}, {"gz": wrap(x + 1, NX)}, {"gz": wrap(x - 1, NX)}]
    for peer in peers:
        pl.semaphore_signal(barrier, inc=1, device_id=peer, device_id_type=MESH)

    own_a = pltpu.make_async_copy(a_hbm, abuf.at[gx], own_sem.at[0])
    own_p = pltpu.make_async_copy(p_hbm, pbuf.at[me], own_sem.at[1])
    own_p.start()
    own_a.start()
    ints = [
        pltpu.make_async_copy(src, dst, int_sem.at[i])
        for i, (src, dst) in enumerate(((ac_hbm, ac), (an_hbm, an), (pc_hbm, pc), (pn_hbm, pn)))
    ]
    for copy in ints:
        copy.start()

    pl.semaphore_wait(barrier, len(peers))

    DIR = {1: 0, -1: 1}
    EARLY = {1: 0, -1: 1}

    def a_part(slot, u):
        return abuf.at[slot, pl.ds(u * UNIT, UNIT)]

    def a_first(d, u, slot):
        return remote(a_part(slot, u), a_part(slot, u), a_send.at[DIR[d]], a_recv.at[DIR[d], u], y_dev(d))

    def a_second(d, slot):
        part = a_part(slot, EARLY[d])
        return remote(part, part, a_send.at[DIR[d]], a_recv.at[DIR[d], 2], y_dev(d))

    def m_copy(hop, d, slot):
        return remote(ameta.at[slot], ameta.at[slot], m_send, m_recv.at[hop], y_dev(d))

    def to_sibling(slot):
        part = abuf.at[slot]
        return remote(part, part, sib_send, sib_recv, sibling)

    def m_sibling(slot):
        return remote(ameta.at[slot], ameta.at[slot], m_send, smeta_recv, sibling)

    def a_start():
        own_a.wait()
        for i in range(2):
            for d in (1, -1):
                a_first(d, EARLY[d] if i == 0 else 1 - EARLY[d], gx).start()
        to_sibling(gx).start()

    def a_near():
        for d in (1, -1):
            a_first(d, EARLY[d], y_slot(-d)).wait_recv()
            a_second(d, y_slot(-d)).start()
        for d in (1, -1):
            m_copy(DIR[d], d, y_slot(-d)).wait_recv()
        m_copy(2, 1, y_slot(-1)).start()
        for d in (1, -1):
            a_first(d, 1 - EARLY[d], y_slot(-d)).wait_recv()
            to_sibling(y_slot(-d)).start()
            m_sibling(y_slot(-d)).start()

    def a_far():
        slot = y_slot(2)
        m_copy(2, 1, slot).wait_recv()
        m_sibling(slot).start()
        for d in (1, -1):
            a_second(d, slot).wait_recv()
        to_sibling(slot).start()

    to_smem = pltpu.make_async_copy(ameta, ameta_s, meta_sem)

    def a_finish():
        part = ameta.at[pl.ds(0, NY)]
        pltpu.make_async_copy(part, part, smeta_recv).wait()
        part = abuf.at[pl.ds(0, NY)]
        pltpu.make_async_copy(part, part, sib_recv).wait()
        to_smem.start()

    def a_drain():
        for d in (0, 1):
            part = abuf.at[pl.ds(0, 3), pl.ds(0, UNIT)]
            pltpu.make_async_copy(part, part, a_send.at[d]).wait()
        part = abuf.at[pl.ds(0, NY)]
        pltpu.make_async_copy(part, part, sib_send).wait()
        part = ameta.at[pl.ds(0, 3 + NY)]
        pltpu.make_async_copy(part, part, m_send).wait()

    PIECES = {1: tuple(range(NP)), -1: tuple(range(NP))[::-1]}
    LAST = {1: tuple(range(NP // 2)), -1: tuple(range(NP // 2, NP))[::-1]}

    def p_part(slot, j):
        return pbuf.at[slot, pl.ds(j * PIECE, PIECE)]

    def p_copy(d, step, j, slot):
        part = p_part(slot, j)
        return remote(
            part, part, p_send.at[DIR[d]], p_recv.at[DIR[d], (step - 1) % DEPTH, j], {"gy": wrap(me + d, NZ)}
        )

    def pm_copy(d, step, slot):
        part = pmeta.at[slot]
        return remote(part, part, pm_send.at[DIR[d]], pm_recv.at[DIR[d], (step - 1) % DEPTH], {"gy": wrap(me + d, NZ)})

    lane = lax.broadcasted_iota(jnp.int32, (TILES_P, T), 1)

    def convert(slot, t):
        p = pbuf[slot, t * T : (t + 1) * T, :]
        packed = pmeta[slot]
        turned = pltpu.roll(packed, T // 2, 1)
        low_half = lane < T // 2
        weights = (jnp.where(low_half, packed, turned), jnp.where(low_half, turned, packed))
        hi = p.astype(BF)
        lo = (p - hi.astype(F32)).astype(BF)
        k = slot * TILES_P + t
        for col in range(2):
            weight = weights[col][t : t + 1, :].astype(BF)
            phi[k, :, col * T : (col + 1) * T] = hi * weight
            plo[k, :, col * T : (col + 1) * T] = lo * weight

    def metas():
        for copy in ints:
            copy.wait()
        row4 = lax.broadcasted_iota(jnp.int32, (TILES_P, T), 0)
        weights = jnp.zeros((TILES_P, T), F32)
        for t in range(TILES_P):
            column = jnp.where(pn[0, t] > 0, pc[0, t], -1)
            named = jnp.where(lane < T // 2, 0, 1) == column
            weights = jnp.where(jnp.logical_and(row4 == t, named), 1.0, weights)
        pmeta[me] = weights
        lane1 = lax.broadcasted_iota(jnp.int32, (1, T), 1)
        targets = jnp.zeros((1, T), jnp.int32)
        for r in range(ROWS_DEV):
            for s in range(SLOTS):
                target = jnp.where(s < an[0, r], ac[0, r, 0, s], NZ * TILES_P)
                targets = jnp.where(lane1 == r * SLOTS + s, target, targets)
        ameta[gx] = targets
        phi[NZ * TILES_P] = jnp.zeros((T, 2 * T), BF)
        plo[NZ * TILES_P] = jnp.zeros((T, 2 * T), BF)
        for d in (1, -1):
            pm_copy(d, 1, me).start()
            m_copy(DIR[d], d, gx).start()
        m_sibling(gx).start()

    def p_send_own(first, last):
        for i in range(first, last):
            for d in (1, -1):
                p_copy(d, 1, PIECES[d][i], me).start()

    def p_start():
        own_p.wait()
        p_send_own(0, NP)

    def p_begin(first, last, held=True):
        def act():
            if first == 0:
                own_p.wait()
            if held:
                pl.semaphore_wait(go_sem, 1)
            p_send_own(first, last)

        return act

    PER = NP // TILES_P

    def spend():
        for d in (1, -1):
            pl.semaphore_wait(credit.at[DIR[d]], 1)

    def give():
        for d in (1, -1):
            pl.semaphore_signal(
                credit.at[DIR[d]], inc=1, device_id={"gy": wrap(me - d, NZ)}, device_id_type=MESH
            )

    def p_steps(first, last):
        def step(s, carry):
            pl.when(s >= DEPTH)(spend)
            for i in range(NP):
                for d in (1, -1):
                    j, slot = PIECES[d][i], wrap(me - d * s, NZ)
                    p_copy(d, s, j, slot).wait_recv()
                    p_copy(d, s + 1, j, slot).start()
                if i % PER == 0:
                    for d in (1, -1):
                        convert(wrap(me - d * (s - 1), NZ), i // PER)
            for d in (1, -1):
                slot = wrap(me - d * s, NZ)
                pm_copy(d, s, slot).wait_recv()
                pm_copy(d, s + 1, slot).start()
            pl.when(s <= HALF - DEPTH)(give)
            return carry

        lax.fori_loop(first, last + 1, step, 0)

    def p_seven():
        s = HALF - 1
        spend()
        for i in range(NP):
            for d in (1, -1):
                j, slot = PIECES[d][i], wrap(me - d * s, NZ)
                p_copy(d, s, j, slot).wait_recv()
                if j in LAST[d]:
                    p_copy(d, HALF, j, slot).start()
            if i % PER == 0:
                for d in (1, -1):
                    convert(wrap(me - d * (s - 1), NZ), i // PER)
        for d in (1, -1):
            slot = wrap(me - d * s, NZ)
            pm_copy(d, s, slot).wait_recv()
            if d == -1:
                pm_copy(d, HALF, slot).start()
        for t in range(TILES_P):
            for d in (1, -1):
                convert(wrap(me - d * s, NZ), t)

    def p_eight():
        slot = wrap(me + HALF, NZ)
        pm_copy(-1, HALF, slot).wait_recv()
        for i in range(NP // 2):
            for d in (1, -1):
                p_copy(d, HALF, LAST[d][i], slot).wait_recv()
            if i % PER == PER - 1:
                for d in (1, -1):
                    convert(slot, LAST[d][i] // PER)

    def p_drain():
        part = pbuf.at[pl.ds(0, 2 * HALF - 1), pl.ds(0, 2 * T)]
        for d in (1, -1):
            pltpu.make_async_copy(part, part, p_send.at[DIR[d]]).wait()
            metas_sent = pmeta.at[pl.ds(0, HALF - 1 if d == 1 else HALF)]
            pltpu.make_async_copy(metas_sent, metas_sent, pm_send.at[DIR[d]]).wait()

    def go():
        pl.semaphore_signal(go_sem, inc=1, device_id=sibling, device_id_type=MESH)

    def follow(plan):
        acts = {
            "P": p_start, "Pa": p_begin(0, 3, False), "Pb": p_begin(3, 6), "Pc": p_begin(6, NP), "A0": a_start, "A1": a_near, "A2": a_far, "A3": a_finish, "M": metas,
            "go": go,
            HALF - 1: p_seven, HALF: p_eight,
        }
        run = []
        for item in plan + (None,):
            if item in range(1, HALF - 1):
                run.append(item)
                continue
            if run:
                p_steps(run[0], run[-1])
                run = []
            if item is not None:
                acts[item]()

    @pl.when(core == 0)
    def _():
        follow(PLAN0)

    @pl.when(core == 1)
    def _():
        follow(PLAN1)

    def compute(o, b):
        row = o * NX + b
        slot, r = row // ROWS_DEV, row % ROWS_DEV
        total = jnp.zeros((T, 2 * T), F32)
        for pair in range(SLOTS // 2):
            left, high, low = [], [], []
            for s in (2 * pair, 2 * pair + 1):
                k = ameta_s[slot, 0, r * SLOTS + s]
                left.append(abuf[slot, r * SLOTS + s])
                high.append(phi[k])
                low.append(plo[k])
            a = jnp.concatenate(left, axis=1)
            hi = a.astype(BF)
            lo = (a - hi.astype(F32)).astype(BF)
            high = jnp.concatenate(high, axis=0)
            low = jnp.concatenate(low, axis=0)
            total += jnp.dot(hi, high, preferred_element_type=F32)
            total += jnp.dot(lo, high, preferred_element_type=F32)
            total += jnp.dot(hi, low, preferred_element_type=F32)
        cbuf[row] = total

    def c_far(d, h, b):
        return remote(cbuf.at[wrap(x + 2, NX) * NX + b], far.at[DIR[d], h], c_send.at[DIR[d]], far_recv.at[DIR[d], h], {"gz": wrap(x + d, NX)})

    def c_near(d, b):
        return remote(cbuf.at[wrap(x + d, NX) * NX + b], near.at[DIR[d], b], c_send.at[DIR[d]], near_recv.at[DIR[d], b], {"gz": wrap(x + d, NX)})

    to_smem.wait()
    opposite, right, left = wrap(x + 2, NX), wrap(x + 1, NX), wrap(x - 1, NX)

    def far_rows(b, carry):
        compute(opposite, b)
        compute(opposite, b + 2)
        c_far(1, b, b).start()
        c_far(-1, b, b + 2).start()
        return carry

    lax.fori_loop(0, 2, far_rows, 0)

    def near_rows(b, carry):
        compute(right, b + 2)
        compute(left, b)
        c_near(1, b + 2).start()
        c_near(-1, b).start()
        return carry

    lax.fori_loop(0, 2, near_rows, 0)

    def near_more(b, carry):
        compute(right, b)
        compute(left, b + 2)
        return carry

    lax.fori_loop(0, 2, near_more, 0)

    def add_far(b, carry):
        c_far(1, b, b).wait_recv()
        cbuf[right * NX + b] += far[0, b]
        c_near(1, b).start()
        c_far(-1, b, b + 2).wait_recv()
        cbuf[left * NX + b + 2] += far[1, b]
        c_near(-1, b + 2).start()
        return carry

    lax.fori_loop(0, 2, add_far, 0)

    def own_rows(b, carry):
        compute(x, b)
        return carry

    lax.fori_loop(0, NX, own_rows, 0)

    def out_copy(b):
        return pltpu.make_async_copy(cbuf.at[x * NX + b], out.at[pl.ds(b * T, T)], out_sem)

    for b in (0, 2, 1, 3):
        for d in (1, -1):
            c_near(d, b).wait_recv()
        cbuf[x * NX + b] += near[0, b] + near[1, b]
        out_copy(b).start()
    p_drain()
    a_drain()
    part = cbuf.at[pl.ds(0, 6)]
    for d in (0, 1):
        pltpu.make_async_copy(part, part, c_send.at[d]).wait()
    part = cbuf.at[pl.ds(0, NX)]
    pltpu.make_async_copy(part, part, out_sem).wait()


def body(a_vals, a_cols, a_count, p_vals, p_cols, p_count):
    a = a_vals.reshape(TILES_A, T, T)
    p = p_vals.reshape(TILES_P * T, T)
    hbm = pl.BlockSpec(memory_space=pltpu.HBM)
    dma = pltpu.SemaphoreType.DMA
    return pl.pallas_call(
        kernel,
        out_shape=jax.ShapeDtypeStruct((NX * T, 2 * T), F32),
        in_specs=[hbm] * 6,
        out_specs=pl.BlockSpec(memory_space=pl.ANY),
        scratch_shapes=[
            pltpu.VMEM((NY * NC, TILES_A, T, T), F32),
            pltpu.VMEM((NY * NC, 1, T), jnp.int32),
            pltpu.SMEM((NY * NC, 1, T), jnp.int32),
            pltpu.SMEM((1, ROWS_DEV, 1, SLOTS), jnp.int32),
            pltpu.SMEM((1, ROWS_DEV), jnp.int32),
            pltpu.SMEM((1, TILES_P), jnp.int32),
            pltpu.SMEM((1, TILES_P), jnp.int32),
            pltpu.VMEM((NZ, PROWS, T), F32),
            pltpu.VMEM((NZ, TILES_P, T), F32),
            pltpu.VMEM((NZ * TILES_P + 1, T, 2 * T), BF),
            pltpu.VMEM((NZ * TILES_P + 1, T, 2 * T), BF),
            pltpu.VMEM((NX * NX, T, 2 * T), F32),
            pltpu.VMEM((2, 2, T, 2 * T), F32),
            pltpu.VMEM((2, NX, T, 2 * T), F32),
            dma((2,)),
            dma((2,)),
            dma((2, DEPTH, NP)),
            dma((2,)),
            dma((2, DEPTH)),
            dma((2,)),
            dma((2, 3)),
            dma,
            dma((3,)),
            dma,
            dma,
            dma,
            dma((2,)),
            dma((2, 2)),
            dma((2, NX)),
            dma,
            dma((4,)),
            dma,
            pltpu.SemaphoreType.REGULAR,
            pltpu.SemaphoreType.REGULAR((2,)),
        ],
        compiler_params=pltpu.CompilerParams(collective_id=0, has_side_effects=True, vmem_limit_bytes=36 * 1024 * 1024),
    )(*(pltpu.with_memory_space_constraint(v, pltpu.HBM) for v in (a, a_cols, a_count.reshape(1, ROWS_DEV), p, p_cols.reshape(1, TILES_P), p_count.reshape(1, TILES_P))))


def solution(mesh):
    placed = (
        P("gy", "gx", "gz", None, None, None),
        P("gy", "gx", "gz", None),
        P("gy", "gx", "gz"),
        P("gz", "gy", "gx", None, None, None),
        P("gz", "gy", "gx", None),
        P("gz", "gy", "gx"),
    )
    return jax.shard_map(body, mesh=mesh, in_specs=placed, out_specs=P(("gy", "gz"), "gx"), check_vma=False)
```

```python
import jax
import jax.numpy as jnp
from jax import lax
from jax.experimental import pallas as pl
from jax.experimental.pallas import tpu as pltpu
from jax.sharding import PartitionSpec as P

MESH = pl.DeviceIdType.MESH
T = 128
NY = 4
NC = 2
NZ = 16
NX = 4
SLOTS = 6
ROWS_DEV = 2
TILES_A = ROWS_DEV * SLOTS
UNIT = TILES_A // 2
TILES_P = 4
PROWS = TILES_P * T
HALF = NZ // 2
NP = 8
DEPTH = 3
PIECE = TILES_P * T // NP
PLAN0 = ("P", "A0", "M", 1, "go", 2, 3, "go", 4, 5, "A1", 6, 7, "A2", 8, "A3")
PLAN1 = ("Pa", "A0", "M", "Pb", "Pc", 1, "A1", 2, 3, "A2", 4, 5, "A3", 6, 7, 8)
BF = jnp.bfloat16
F32 = jnp.float32


def kernel(
    a_hbm, ac_hbm, an_hbm, p_hbm, pc_hbm, pn_hbm, out,
    abuf, ameta, ameta_s, ac, an, pc, pn, pbuf, pmeta, phi, plo, cbuf, far, near,
    own_sem, p_send, p_recv, pm_send, pm_recv, a_send, a_recv, m_send, m_recv,
    sib_send, sib_recv, smeta_recv, c_send, far_recv, near_recv, out_sem, int_sem, meta_sem, go_sem, credit,
):
    gx, me, x = lax.axis_index("gx"), lax.axis_index("gy"), lax.axis_index("gz")
    y, core = gx // NC, gx % NC

    def wrap(value, n):
        return lax.rem(value + 2 * n, n)

    def y_dev(d):
        return {"gx": wrap(y + d, NY) * NC + core}

    def y_slot(d):
        return wrap(y + d, NY) * NC + core

    sibling = {"gx": y * NC + 1 - core}

    def remote(src, dst, send, recv, device):
        return pltpu.make_async_remote_copy(
            src_ref=src, dst_ref=dst, send_sem=send, recv_sem=recv, device_id=device, device_id_type=MESH
        )

    barrier = pltpu.get_barrier_semaphore()
    peers = [sibling, y_dev(1), y_dev(-1), {"gy": wrap(me + 1, NZ)}, {"gy": wrap(me - 1, NZ)}, {"gz": wrap(x + 1, NX)}, {"gz": wrap(x - 1, NX)}]
    for peer in peers:
        pl.semaphore_signal(barrier, inc=1, device_id=peer, device_id_type=MESH)

    own_a = pltpu.make_async_copy(a_hbm, abuf.at[gx], own_sem.at[0])
    own_p = pltpu.make_async_copy(p_hbm, pbuf.at[me], own_sem.at[1])
    own_p.start()
    own_a.start()
    ints = [
        pltpu.make_async_copy(src, dst, int_sem.at[i])
        for i, (src, dst) in enumerate(((ac_hbm, ac), (an_hbm, an), (pc_hbm, pc), (pn_hbm, pn)))
    ]
    for copy in ints:
        copy.start()

    pl.semaphore_wait(barrier, len(peers))

    DIR = {1: 0, -1: 1}
    EARLY = {1: 0, -1: 1}

    def a_part(slot, u):
        return abuf.at[slot, pl.ds(u * UNIT, UNIT)]

    def a_first(d, u, slot):
        return remote(a_part(slot, u), a_part(slot, u), a_send.at[DIR[d]], a_recv.at[DIR[d], u], y_dev(d))

    def a_second(d, slot):
        part = a_part(slot, EARLY[d])
        return remote(part, part, a_send.at[DIR[d]], a_recv.at[DIR[d], 2], y_dev(d))

    def m_copy(hop, d, slot):
        return remote(ameta.at[slot], ameta.at[slot], m_send, m_recv.at[hop], y_dev(d))

    def to_sibling(slot):
        part = abuf.at[slot]
        return remote(part, part, sib_send, sib_recv, sibling)

    def m_sibling(slot):
        return remote(ameta.at[slot], ameta.at[slot], m_send, smeta_recv, sibling)

    def a_start():
        own_a.wait()
        for i in range(2):
            for d in (1, -1):
                a_first(d, EARLY[d] if i == 0 else 1 - EARLY[d], gx).start()
        to_sibling(gx).start()

    def a_near():
        for d in (1, -1):
            a_first(d, EARLY[d], y_slot(-d)).wait_recv()
            a_second(d, y_slot(-d)).start()
        for d in (1, -1):
            m_copy(DIR[d], d, y_slot(-d)).wait_recv()
        m_copy(2, 1, y_slot(-1)).start()
        for d in (1, -1):
            a_first(d, 1 - EARLY[d], y_slot(-d)).wait_recv()
            to_sibling(y_slot(-d)).start()
            m_sibling(y_slot(-d)).start()

    def a_far():
        slot = y_slot(2)
        m_copy(2, 1, slot).wait_recv()
        m_sibling(slot).start()
        for d in (1, -1):
            a_second(d, slot).wait_recv()
        to_sibling(slot).start()

    to_smem = pltpu.make_async_copy(ameta, ameta_s, meta_sem)

    def a_finish():
        part = ameta.at[pl.ds(0, NY)]
        pltpu.make_async_copy(part, part, smeta_recv).wait()
        part = abuf.at[pl.ds(0, NY)]
        pltpu.make_async_copy(part, part, sib_recv).wait()
        to_smem.start()

    def a_drain():
        for d in (0, 1):
            part = abuf.at[pl.ds(0, 3), pl.ds(0, UNIT)]
            pltpu.make_async_copy(part, part, a_send.at[d]).wait()
        part = abuf.at[pl.ds(0, NY)]
        pltpu.make_async_copy(part, part, sib_send).wait()
        part = ameta.at[pl.ds(0, 3 + NY)]
        pltpu.make_async_copy(part, part, m_send).wait()

    PIECES = {1: tuple(range(NP)), -1: tuple(range(NP))[::-1]}
    LAST = {1: tuple(range(NP // 2)), -1: tuple(range(NP // 2, NP))[::-1]}

    def p_part(slot, j):
        return pbuf.at[slot, pl.ds(j * PIECE, PIECE)]

    def p_copy(d, step, j, slot):
        part = p_part(slot, j)
        return remote(
            part, part, p_send.at[DIR[d]], p_recv.at[DIR[d], (step - 1) % DEPTH, j], {"gy": wrap(me + d, NZ)}
        )

    def pm_copy(d, step, slot):
        part = pmeta.at[slot]
        return remote(part, part, pm_send.at[DIR[d]], pm_recv.at[DIR[d], (step - 1) % DEPTH], {"gy": wrap(me + d, NZ)})

    lane = lax.broadcasted_iota(jnp.int32, (TILES_P, T), 1)

    def convert(slot, t):
        p = pbuf[slot, t * T : (t + 1) * T, :]
        packed = pmeta[slot]
        turned = pltpu.roll(packed, T // 2, 1)
        low_half = lane < T // 2
        weights = (jnp.where(low_half, packed, turned), jnp.where(low_half, turned, packed))
        hi = p.astype(BF)
        lo = (p - hi.astype(F32)).astype(BF)
        k = slot * TILES_P + t
        for col in range(2):
            weight = weights[col][t : t + 1, :].astype(BF)
            phi[k, :, col * T : (col + 1) * T] = hi * weight
            plo[k, :, col * T : (col + 1) * T] = lo * weight

    def metas():
        for copy in ints:
            copy.wait()
        row4 = lax.broadcasted_iota(jnp.int32, (TILES_P, T), 0)
        weights = jnp.zeros((TILES_P, T), F32)
        for t in range(TILES_P):
            column = jnp.where(pn[0, t] > 0, pc[0, t], -1)
            named = jnp.where(lane < T // 2, 0, 1) == column
            weights = jnp.where(jnp.logical_and(row4 == t, named), 1.0, weights)
        pmeta[me] = weights
        lane1 = lax.broadcasted_iota(jnp.int32, (1, T), 1)
        targets = jnp.zeros((1, T), jnp.int32)
        for r in range(ROWS_DEV):
            for s in range(SLOTS):
                target = jnp.where(s < an[0, r], ac[0, r, 0, s], NZ * TILES_P)
                targets = jnp.where(lane1 == r * SLOTS + s, target, targets)
        ameta[gx] = targets
        phi[NZ * TILES_P] = jnp.zeros((T, 2 * T), BF)
        plo[NZ * TILES_P] = jnp.zeros((T, 2 * T), BF)
        for d in (1, -1):
            pm_copy(d, 1, me).start()
            m_copy(DIR[d], d, gx).start()
        m_sibling(gx).start()

    def p_send_own(first, last):
        for i in range(first, last):
            for d in (1, -1):
                p_copy(d, 1, PIECES[d][i], me).start()

    def p_start():
        own_p.wait()
        p_send_own(0, NP)

    def p_begin(first, last, held=True):
        def act():
            if first == 0:
                own_p.wait()
            if held:
                pl.semaphore_wait(go_sem, 1)
            p_send_own(first, last)

        return act

    PER = NP // TILES_P

    def spend():
        for d in (1, -1):
            pl.semaphore_wait(credit.at[DIR[d]], 1)

    def give():
        for d in (1, -1):
            pl.semaphore_signal(
                credit.at[DIR[d]], inc=1, device_id={"gy": wrap(me - d, NZ)}, device_id_type=MESH
            )

    def p_steps(first, last):
        def step(s, carry):
            pl.when(s >= DEPTH)(spend)
            for i in range(NP):
                for d in (1, -1):
                    j, slot = PIECES[d][i], wrap(me - d * s, NZ)
                    p_copy(d, s, j, slot).wait_recv()
                    p_copy(d, s + 1, j, slot).start()
                if i % PER == 0:
                    for d in (1, -1):
                        convert(wrap(me - d * (s - 1), NZ), i // PER)
            for d in (1, -1):
                slot = wrap(me - d * s, NZ)
                pm_copy(d, s, slot).wait_recv()
                pm_copy(d, s + 1, slot).start()
            pl.when(s <= HALF - DEPTH)(give)
            return carry

        lax.fori_loop(first, last + 1, step, 0)

    def p_seven():
        s = HALF - 1
        spend()
        for i in range(NP):
            for d in (1, -1):
                j, slot = PIECES[d][i], wrap(me - d * s, NZ)
                p_copy(d, s, j, slot).wait_recv()
                if j in LAST[d]:
                    p_copy(d, HALF, j, slot).start()
            if i % PER == 0:
                for d in (1, -1):
                    convert(wrap(me - d * (s - 1), NZ), i // PER)
        for d in (1, -1):
            slot = wrap(me - d * s, NZ)
            pm_copy(d, s, slot).wait_recv()
            if d == -1:
                pm_copy(d, HALF, slot).start()
        for t in range(TILES_P):
            for d in (1, -1):
                convert(wrap(me - d * s, NZ), t)

    def p_eight():
        slot = wrap(me + HALF, NZ)
        pm_copy(-1, HALF, slot).wait_recv()
        for i in range(NP // 2):
            for d in (1, -1):
                p_copy(d, HALF, LAST[d][i], slot).wait_recv()
            if i % PER == PER - 1:
                for d in (1, -1):
                    convert(slot, LAST[d][i] // PER)

    def p_drain():
        part = pbuf.at[pl.ds(0, 2 * HALF - 1), pl.ds(0, 2 * T)]
        for d in (1, -1):
            pltpu.make_async_copy(part, part, p_send.at[DIR[d]]).wait()
            metas_sent = pmeta.at[pl.ds(0, HALF - 1 if d == 1 else HALF)]
            pltpu.make_async_copy(metas_sent, metas_sent, pm_send.at[DIR[d]]).wait()

    def go():
        pl.semaphore_signal(go_sem, inc=1, device_id=sibling, device_id_type=MESH)

    def follow(plan):
        acts = {
            "P": p_start, "Pa": p_begin(0, 4, False), "Pb": p_begin(4, 6), "Pc": p_begin(6, NP), "A0": a_start, "A1": a_near, "A2": a_far, "A3": a_finish, "M": metas,
            "go": go,
            HALF - 1: p_seven, HALF: p_eight,
        }
        run = []
        for item in plan + (None,):
            if item in range(1, HALF - 1):
                run.append(item)
                continue
            if run:
                p_steps(run[0], run[-1])
                run = []
            if item is not None:
                acts[item]()

    @pl.when(core == 0)
    def _():
        follow(PLAN0)

    @pl.when(core == 1)
    def _():
        follow(PLAN1)

    def compute(o, b):
        row = o * NX + b
        slot, r = row // ROWS_DEV, row % ROWS_DEV
        total = jnp.zeros((T, 2 * T), F32)
        for pair in range(SLOTS // 2):
            left, high, low = [], [], []
            for s in (2 * pair, 2 * pair + 1):
                k = ameta_s[slot, 0, r * SLOTS + s]
                left.append(abuf[slot, r * SLOTS + s])
                high.append(phi[k])
                low.append(plo[k])
            a = jnp.concatenate(left, axis=1)
            hi = a.astype(BF)
            lo = (a - hi.astype(F32)).astype(BF)
            high = jnp.concatenate(high, axis=0)
            low = jnp.concatenate(low, axis=0)
            total += jnp.dot(hi, high, preferred_element_type=F32)
            total += jnp.dot(lo, high, preferred_element_type=F32)
            total += jnp.dot(hi, low, preferred_element_type=F32)
        cbuf[row] = total

    def c_far(d, h, b):
        return remote(cbuf.at[wrap(x + 2, NX) * NX + b], far.at[DIR[d], h], c_send.at[DIR[d]], far_recv.at[DIR[d], h], {"gz": wrap(x + d, NX)})

    def c_near(d, b):
        return remote(cbuf.at[wrap(x + d, NX) * NX + b], near.at[DIR[d], b], c_send.at[DIR[d]], near_recv.at[DIR[d], b], {"gz": wrap(x + d, NX)})

    to_smem.wait()
    opposite, right, left = wrap(x + 2, NX), wrap(x + 1, NX), wrap(x - 1, NX)

    def far_rows(b, carry):
        compute(opposite, b)
        compute(opposite, b + 2)
        c_far(1, b, b).start()
        c_far(-1, b, b + 2).start()
        return carry

    lax.fori_loop(0, 2, far_rows, 0)

    def near_rows(b, carry):
        compute(right, b + 2)
        compute(left, b)
        c_near(1, b + 2).start()
        c_near(-1, b).start()
        return carry

    lax.fori_loop(0, 2, near_rows, 0)

    def near_more(b, carry):
        compute(right, b)
        compute(left, b + 2)
        return carry

    lax.fori_loop(0, 2, near_more, 0)

    def add_far(b, carry):
        c_far(1, b, b).wait_recv()
        cbuf[right * NX + b] += far[0, b]
        c_near(1, b).start()
        c_far(-1, b, b + 2).wait_recv()
        cbuf[left * NX + b + 2] += far[1, b]
        c_near(-1, b + 2).start()
        return carry

    lax.fori_loop(0, 2, add_far, 0)

    def own_rows(b, carry):
        compute(x, b)
        return carry

    lax.fori_loop(0, NX, own_rows, 0)

    def out_copy(b):
        return pltpu.make_async_copy(cbuf.at[x * NX + b], out.at[pl.ds(b * T, T)], out_sem)

    for b in (0, 2, 1, 3):
        for d in (1, -1):
            c_near(d, b).wait_recv()
        cbuf[x * NX + b] += near[0, b] + near[1, b]
        out_copy(b).start()
    p_drain()
    a_drain()
    part = cbuf.at[pl.ds(0, 6)]
    for d in (0, 1):
        pltpu.make_async_copy(part, part, c_send.at[d]).wait()
    part = cbuf.at[pl.ds(0, NX)]
    pltpu.make_async_copy(part, part, out_sem).wait()


def body(a_vals, a_cols, a_count, p_vals, p_cols, p_count):
    a = a_vals.reshape(TILES_A, T, T)
    p = p_vals.reshape(TILES_P * T, T)
    hbm = pl.BlockSpec(memory_space=pltpu.HBM)
    dma = pltpu.SemaphoreType.DMA
    return pl.pallas_call(
        kernel,
        out_shape=jax.ShapeDtypeStruct((NX * T, 2 * T), F32),
        in_specs=[hbm] * 6,
        out_specs=pl.BlockSpec(memory_space=pl.ANY),
        scratch_shapes=[
            pltpu.VMEM((NY * NC, TILES_A, T, T), F32),
            pltpu.VMEM((NY * NC, 1, T), jnp.int32),
            pltpu.SMEM((NY * NC, 1, T), jnp.int32),
            pltpu.SMEM((1, ROWS_DEV, 1, SLOTS), jnp.int32),
            pltpu.SMEM((1, ROWS_DEV), jnp.int32),
            pltpu.SMEM((1, TILES_P), jnp.int32),
            pltpu.SMEM((1, TILES_P), jnp.int32),
            pltpu.VMEM((NZ, PROWS, T), F32),
            pltpu.VMEM((NZ, TILES_P, T), F32),
            pltpu.VMEM((NZ * TILES_P + 1, T, 2 * T), BF),
            pltpu.VMEM((NZ * TILES_P + 1, T, 2 * T), BF),
            pltpu.VMEM((NX * NX, T, 2 * T), F32),
            pltpu.VMEM((2, 2, T, 2 * T), F32),
            pltpu.VMEM((2, NX, T, 2 * T), F32),
            dma((2,)),
            dma((2,)),
            dma((2, DEPTH, NP)),
            dma((2,)),
            dma((2, DEPTH)),
            dma((2,)),
            dma((2, 3)),
            dma,
            dma((3,)),
            dma,
            dma,
            dma,
            dma((2,)),
            dma((2, 2)),
            dma((2, NX)),
            dma,
            dma((4,)),
            dma,
            pltpu.SemaphoreType.REGULAR,
            pltpu.SemaphoreType.REGULAR((2,)),
        ],
        compiler_params=pltpu.CompilerParams(collective_id=0, has_side_effects=True, vmem_limit_bytes=36 * 1024 * 1024),
    )(*(pltpu.with_memory_space_constraint(v, pltpu.HBM) for v in (a, a_cols, a_count.reshape(1, ROWS_DEV), p, p_cols.reshape(1, TILES_P), p_count.reshape(1, TILES_P))))


def solution(mesh):
    placed = (
        P("gy", "gx", "gz", None, None, None),
        P("gy", "gx", "gz", None),
        P("gy", "gx", "gz"),
        P("gz", "gy", "gx", None, None, None),
        P("gz", "gy", "gx", None),
        P("gz", "gy", "gx"),
    )
    return jax.shard_map(body, mesh=mesh, in_specs=placed, out_specs=P(("gy", "gz"), "gx"), check_vma=False)
```
